256 devices in a mesh: dp: 4 (over x), expert: 64 (over z, y, core).
Axes of the slice: x: 4, y: 4, z: 8, core: 2. Of those that a mesh axis runs over, the one named last changes fastest.
Arguments:
- tokens: bfloat16 [32768, 2048], P(('dp', 'expert')), may hold values from -6 to 6
- expert_ids: int32 [32768, 2], P(('dp', 'expert')), may hold values from 0 to 63, all different within a row; in each aligned block of 128 rows (0 to 127, 128 to 255, ...) at most 5 rows name the same one
- gate_units: int32 [32768, 2], P(('dp', 'expert')), may hold values from 64 to 1023
- capacity: int32 [64], replicated, may hold values from 512 to 1535
- w_gate: bfloat16 [64, 2048, 1408], P('expert', None, 'dp'), may hold values from -0.125 to 0.125
- w_up: bfloat16 [64, 2048, 1408], P('expert', None, 'dp'), may hold values from -0.125 to 0.125
- w_down: bfloat16 [64, 2048, 1408], P('expert', None, 'dp'), may hold values from -0.15625 to 0.15625
Outputs:
- mixed: bfloat16 [32768, 2048], P(('dp', 'expert'))
The draws below stay inside these ranges and needn't reach their ends.
Inputs may be any that keep to these rules, and one draw needn't show every extreme that they name: `expert_ids`: each row names two different experts; of one device's 128 rows (aligned blocks) no expert is named more than 5 times.
All inputs are finite; a program needn't handle non-finite values.
Results may differ from the reference program's by a relative error of at most 0.0057.
Values may be sent and summed in bfloat16 or wider, within the bound.
A program may use at most 128 MiB of HBM per device.

```python
import math
import jax
import jax.numpy as jnp
import numpy as np
from jax import lax

D = 2048
FF = 1408
TOK_DEV = 128
EXPERTS = 64
TOKENS = 32768
MOST = 5
CAP_HI = 1536


def touch_ends(values, key, low, top_value):
    place = [jax.random.randint(jax.random.fold_in(key, axis), (), 0, length) for axis, length in enumerate(values.shape)]
    main_axis = values.shape.index(max(values.shape))
    neighbour = place[:main_axis] + [(place[main_axis] + 1) % values.shape[main_axis]] + place[main_axis + 1:]
    return values.at[tuple(place)].set(low).at[tuple(neighbour)].set(top_value)


def level_of(key, shape, split, smallest, top_value):
    loudness, own = 1.0, jax.random.fold_in(key, 6)
    for position, shards_of in split:
        heights = jnp.exp(jax.random.uniform(jax.random.fold_in(own, position), (shards_of,), jnp.float32, smallest / len(split), top_value / len(split)))
        loudness = loudness * jnp.repeat(heights, shape[position] // shards_of).reshape([-1 if axis == position else 1 for axis in range(len(shape))])
    return loudness


def routed_block(key, own, number, rows, number_of, top, limit, lean):
    sequence = jax.random.permutation(key, number_of)
    packed, ordinary = load_shares(number_of, rows * top, limit, lean, True), load_shares(number_of, rows * top, limit, lean, False)
    places = jnp.arange(number_of)

    def named(lengths, turn):
        used = int((lengths > 0).sum())
        fixed = max(1, used // 4)
        shifted = fixed + (places - fixed + turn * (used - fixed)) % max(1, number_of - fixed)
        return jnp.zeros((number_of,), jnp.int32).at[sequence[jnp.where(places < fixed, places, shifted)]].set(jnp.asarray(lengths, jnp.int32))

    lengths = jnp.where(number % 4 == 0, named(packed, number // 4), named(ordinary, number - number // 4 - 1))
    mixed = jax.random.permutation(jax.random.fold_in(own, 3), number_of)
    giver, taker = mixed[0:number_of // 2 * 2:2], mixed[1:number_of // 2 * 2:2]
    room = jnp.minimum(lengths[giver] - 1, limit - lengths[taker]) // 2
    room = jnp.where((giver == sequence[0]) | (taker == sequence[0]) | (lengths[taker] == 0), 0, jnp.maximum(room, 0))
    shifted = jax.random.randint(jax.random.fold_in(own, 4), (number_of // 2,), 0, 1 << 20) % (room + 1)
    lengths = lengths.at[giver].add(-shifted).at[taker].add(shifted)
    items = jnp.searchsorted(jnp.cumsum(lengths), jnp.arange(rows * top), side="right").astype(jnp.int32)
    listing = items.reshape(top, rows).T
    listing = listing[jax.random.permutation(jax.random.fold_in(own, 1), rows)]
    turn = jax.random.randint(jax.random.fold_in(own, 2), (rows, 1), 0, top)
    return jnp.take_along_axis(listing, (jnp.arange(top)[None, :] + turn) % top, axis=1)


def load_shares(amount, total, limit, skew, full):
    weights = [(1 << 20) // math.isqrt(standing ** skew) + 1 for standing in range(1, amount + 1)]
    largest = limit if full else min(limit, max(-(-total // amount), total * weights[0] // sum(weights)))
    least = 1 if total - largest >= amount - 1 else 0
    counts, spare = [largest] + [least] * (amount - 1), total - largest - least * (amount - 1)
    while spare > 0:
        movable = [i for i in range(1, amount) if counts[i] < largest] or [i for i in range(1, amount) if counts[i] < limit]
        whole, left = sum([weights[i] for i in movable]), spare
        for i in movable:
            extra = min(limit - counts[i], max(1, left * weights[i] // whole), spare)
            counts[i] = counts[i] + extra
            spare = spare - extra
    return np.array(counts)


def noise(key, dims, width, limit, shards=(), kind=jnp.bfloat16):
    loudness = level_of(key, dims, shards, -0.22, 0.18) if shards else 1.0
    values = jax.random.normal(key, dims, jnp.float32) * width * loudness
    return jnp.minimum(jnp.maximum(values, -limit), limit).astype(kind)


def setup_inputs(seed: int = 0) -> dict:
    arg_keys = jax.random.split(jax.random.key(seed), 8)
    tokens = noise(arg_keys[0], (TOKENS, D), 1.0, 6.0, ((0, 256),))
    expert_ids_keys = jax.random.split(jax.random.fold_in(arg_keys[1], 1), TOKENS // TOK_DEV)
    expert_ids_turns = jax.random.permutation(jax.random.fold_in(arg_keys[1], 3), TOKENS // TOK_DEV)
    expert_ids = jax.vmap(lambda own, number: routed_block(jax.random.fold_in(arg_keys[1], 2), own, number, TOK_DEV, EXPERTS, 2, MOST, 1))(expert_ids_keys, expert_ids_turns).reshape((TOKENS, 2))
    gate_units = touch_ends(jax.random.randint(arg_keys[2], (TOKENS, 2), 64, 1024), jax.random.fold_in(arg_keys[2], 1), 64, 1023).astype(jnp.int32)
    capacity = touch_ends(jax.random.randint(arg_keys[3], (EXPERTS,), TOKENS // EXPERTS, CAP_HI), jax.random.fold_in(arg_keys[3], 1), TOKENS // EXPERTS, CAP_HI - 1).astype(jnp.int32)
    w_gate = noise(arg_keys[4], (EXPERTS, D, FF), D ** -0.5, 0.125, ((0, 64), (2, 4)))
    w_up = noise(arg_keys[5], (EXPERTS, D, FF), D ** -0.5, 0.125, ((0, 64), (2, 4)))
    w_down = noise(arg_keys[6], (EXPERTS, D, FF), FF ** -0.5, 0.15625, ((0, 64), (2, 4)))
    return {"tokens": tokens, "expert_ids": expert_ids, "gate_units": gate_units, "capacity": capacity, "w_gate": w_gate, "w_up": w_up, "w_down": w_down}


def expert_rows(rows, gate_w, up_w, down_w):
    gate = jnp.dot(rows, gate_w, preferred_element_type=jnp.float32)
    up = jnp.dot(rows, up_w, preferred_element_type=jnp.float32)
    hidden = (jax.nn.silu(gate) * up).astype(jnp.bfloat16)
    return lax.dot_general(hidden, down_w, (((1,), (1,)), ((), ())), preferred_element_type=jnp.float32)


def reference(tokens, expert_ids, gate_units, capacity, w_gate, w_up, w_down):
    flat = expert_ids.reshape(-1).astype(jnp.int32)
    onehot = (flat[:, None] == jnp.arange(EXPERTS, dtype=jnp.int32)[None, :]).astype(jnp.int32)
    slot = jnp.sum((jnp.cumsum(onehot, axis=0) - onehot) * onehot, axis=1).astype(jnp.int32)
    kept = slot < capacity[flat]
    weight = jnp.where(kept, gate_units.reshape(-1).astype(jnp.float32) / 1024.0, jnp.float32(0.0))
    token_of = (jnp.arange(2 * TOKENS, dtype=jnp.int32) // 2).astype(jnp.int32)

    def per_expert(carry, index):
        target = jnp.where((flat == index) & kept, slot, CAP_HI).astype(jnp.int32)
        rows_index = jnp.zeros((CAP_HI,), jnp.int32).at[target].set(token_of, mode="drop")
        scales = jnp.zeros((CAP_HI,), jnp.float32).at[target].set(weight, mode="drop")
        result = expert_rows(tokens[rows_index], w_gate[index], w_up[index], w_down[index])
        result = result.astype(jnp.bfloat16).astype(jnp.float32)
        carry = carry.at[rows_index].add(result * scales[:, None])
        return carry, None

    total, _ = lax.scan(per_expert, jnp.zeros((TOKENS, D), jnp.float32), jnp.arange(EXPERTS, dtype=jnp.int32))
    return total.astype(jnp.bfloat16)
```

```python
import functools

import jax
import jax.numpy as jnp
from jax import lax
from jax.experimental import pallas as pl
from jax.experimental.pallas import tpu as pltpu
from jax.sharding import Mesh
from jax.sharding import PartitionSpec as P

MESH = pl.DeviceIdType.MESH
AXES = ("dp", "expert_0", "expert_1", "expert_2")
EXPERT = ("expert_0", "expert_1", "expert_2")
BF16, F32, I32 = jnp.bfloat16, jnp.float32, jnp.int32
LANES = 128
ROW_TILE = 16


def z_groups(nz):
    half = nz // 2
    pairs = [(0, 1)] + [(-k, k + 1) for k in range(1, half)]
    return pairs[:1] + pairs[2:] + pairs[1:2]


def log2(n):
    assert n & (n - 1) == 0
    return n.bit_length() - 1


def kernel(
    shape, most,
    tokens, ids, units, cap, wg_h, wu_h, wd_h, out,
    wg, wu, wd, perm, rows2d, out3, recv3, ret3, back3, a2d, hid, own, pf, part, rs1, rs2,
    sel, whi, wlo, acc, cnt_mine, cnt_all, tot_mine, tot_all,
    w_sem, a2a_send, a2a_recv, ag_send, ag_recv, rs_send, rs_recv, back_send, back_recv, cnt_send, cnt_recv, tot_send, tot_recv,
):
    nx, nz, ny, nc = shape
    x, z, y, c = (lax.axis_index(a) for a in AXES)
    right, left, opp = lax.rem(x + 1, nx), lax.rem(x + nx - 1, nx), lax.rem(x + 2, nx)
    plane = nz * ny * nc
    per_z = ny * nc
    groups = z_groups(nz)
    per_group = 2 * per_z
    gr = per_group * most
    blocks = gr // ROW_TILE
    t_rows, width = tokens.shape
    half = width // 2
    lo, hi = pl.ds(0, half), pl.ds(half, half)

    def at_x(new_x):
        return (new_x, z, y, c)

    def relative(sign, dz, dy, dc):
        return (
            x,
            lax.rem(z + sign * dz + 2 * nz, nz),
            lax.rem(y + sign * dy + ny, ny),
            lax.rem(c + sign * dc + nc, nc),
        )

    def split(i):
        return i // per_z, lax.rem(i // nc, ny), lax.rem(i, nc)

    barrier = pltpu.get_barrier_semaphore()

    def greet(i, carry):
        pl.semaphore_signal(barrier, inc=1, device_id=relative(1, *split(i)), device_id_type=MESH)
        return carry

    for new_x in (right, left, opp):
        pl.semaphore_signal(barrier, inc=1, device_id=at_x(new_x), device_id_type=MESH)
    lax.fori_loop(1, plane, greet, 0)

    loads = [
        pltpu.make_async_copy(src.at[0], dst, w_sem.at[i])
        for i, (src, dst) in enumerate(((wg_h, wg), (wu_h, wu), (wd_h, wd)))
    ]
    for load in loads:
        load.start()

    lane = lax.broadcasted_iota(I32, (t_rows, LANES), 1)
    id0, id1 = ids[:, 0:1], ids[:, 1:2]
    oh0, oh1 = (lane == id0).astype(F32), (lane == id1).astype(F32)
    named = oh0 + oh1
    counts = jnp.sum(named, axis=0, keepdims=True)
    cnt_mine[...] = counts
    cnt_all[0] = counts
    earlier = (
        lax.broadcasted_iota(I32, (t_rows, t_rows), 1) < lax.broadcasted_iota(I32, (t_rows, t_rows), 0)
    ).astype(BF16)
    before = jnp.dot(earlier, named.astype(BF16), preferred_element_type=F32)
    rank0 = jnp.sum(before * oh0, axis=1, keepdims=True)
    rank1 = jnp.sum(before * oh1, axis=1, keepdims=True)

    def slot_of(expert, rank):
        ez = lax.shift_right_logical(expert, log2(per_z))
        ey = lax.shift_right_logical(expert, log2(nc)) & (ny - 1)
        ec = expert & (nc - 1)
        dz = (ez - z + nz) & (nz - 1)
        dy = (ey - y + ny) & (ny - 1)
        dc = (ec - c + nc) & (nc - 1)
        place = jnp.zeros_like(dz)
        for g, pair in enumerate(groups):
            for zi, off in enumerate(pair):
                place = jnp.where(dz == off % nz, 2 * g + zi, place)
        return (place * per_z + dy * nc + dc) * most + rank.astype(I32)

    pos0, pos1 = slot_of(id0, rank0), slot_of(id1, rank1)

    i_row = lax.broadcasted_iota(I32, (256, 256), 0)
    i_col = lax.broadcasted_iota(I32, (256, 256), 1)
    swapped = (i_row & 15) * 16 + lax.shift_right_logical(i_row, 4)
    perm[...] = (i_col == swapped).astype(BF16)

    def to_tiles(dst3, g):
        for b in range(blocks):
            block = rows2d[ROW_TILE * b : ROW_TILE * (b + 1), :]
            stacked = jnp.concatenate(
                [block[:, LANES * s : LANES * (s + 1)] for s in range(width // LANES)], axis=0
            )
            turned = jnp.dot(perm[...], stacked, preferred_element_type=F32).astype(BF16)
            r = g * gr + ROW_TILE * b
            dst3[r : r + ROW_TILE] = turned.reshape(ROW_TILE, ROW_TILE, LANES)

    def from_tiles(src3, g, dst):
        for b in range(blocks):
            r = g * gr + ROW_TILE * b
            stacked = src3[r : r + ROW_TILE].reshape(ROW_TILE * ROW_TILE, LANES)
            turned = jnp.dot(perm[...], stacked, preferred_element_type=F32).astype(BF16)
            for s in range(width // LANES):
                dst[ROW_TILE * b : ROW_TILE * (b + 1), LANES * s : LANES * (s + 1)] = turned[
                    ROW_TILE * s : ROW_TILE * (s + 1), :
                ]

    def exchange(src, dst, g, sign, send_sem, recv_sem):
        a, b = groups[g]
        first = 1 if a == 0 else 0
        base = g * per_group

        def one(i, carry):
            zi, dy, dc = split(i)
            rows = pl.ds((base + i) * most, most)
            pltpu.make_async_remote_copy(
                src_ref=src.at[rows],
                dst_ref=dst.at[rows],
                send_sem=send_sem.at[g],
                recv_sem=recv_sem.at[g],
                device_id=relative(sign, a + zi * (b - a), dy, dc),
                device_id_type=MESH,
            ).start()
            return carry

        lax.fori_loop(first, per_group, one, 0)
        if first:
            dst[base * most : (base + 1) * most] = src[base * most : (base + 1) * most]

    def exchanged(ref, g, sem):
        first = 1 if groups[g][0] == 0 else 0
        rows = pl.ds((g * per_group + first) * most, (per_group - first) * most)
        pltpu.make_async_copy(ref.at[rows], ref.at[rows], sem.at[g]).wait()

    slots = lax.broadcasted_iota(I32, (t_rows, gr), 1)

    def gather(g):
        s0, s1 = (slots + g * gr == pos0), (slots + g * gr == pos1)
        chosen = (s0.astype(F32) + s1.astype(F32)).astype(BF16)
        rows = lax.dot_general(
            chosen, tokens[...], (((0,), (0,)), ((), ())), preferred_element_type=F32
        )
        rows2d[...] = rows.astype(BF16)
        to_tiles(out3, g)

    sent = []

    def push(src, dst, send_sem, recv_sem, new_x):
        copy = pltpu.make_async_remote_copy(
            src_ref=src, dst_ref=dst, send_sem=send_sem, recv_sem=recv_sem,
            device_id=at_x(new_x), device_id_type=MESH,
        )
        copy.start()
        sent.append(copy)

    def arrive(ref, sem):
        pltpu.make_async_copy(ref, ref, sem).wait()

    def rows_of(slot):
        return pl.ds(slot * gr, gr)

    def s1(g):
        exchanged(recv3, g, a2a_recv)
        from_tiles(recv3, g, a2d.at[g])
        me = rows_of(0)
        push(a2d.at[g, me, lo], a2d.at[g, rows_of(1), lo], ag_send.at[g, 0], ag_recv.at[g, 0], right)
        push(a2d.at[g, me, hi], a2d.at[g, rows_of(2), hi], ag_send.at[g, 1], ag_recv.at[g, 1], left)
        push(a2d.at[g, me, hi], a2d.at[g, rows_of(1), hi], ag_send.at[g, 2], ag_recv.at[g, 2], right)
        push(a2d.at[g, me, lo], a2d.at[g, rows_of(2), lo], ag_send.at[g, 3], ag_recv.at[g, 3], left)

    def s2(g):
        arrive(a2d.at[g, rows_of(1), lo], ag_recv.at[g, 0])
        push(a2d.at[g, rows_of(1), lo], a2d.at[g, rows_of(3), lo], ag_send.at[g, 4], ag_recv.at[g, 4], right)
        arrive(a2d.at[g, rows_of(2), hi], ag_recv.at[g, 1])
        push(a2d.at[g, rows_of(2), hi], a2d.at[g, rows_of(3), hi], ag_send.at[g, 5], ag_recv.at[g, 5], left)

    def s3(g):
        arrive(a2d.at[g, rows_of(1), hi], ag_recv.at[g, 2])
        arrive(a2d.at[g, rows_of(2), lo], ag_recv.at[g, 3])
        arrive(a2d.at[g, rows_of(3), lo], ag_recv.at[g, 4])
        arrive(a2d.at[g, rows_of(3), hi], ag_recv.at[g, 5])
        if g == 0:
            for load in loads:
                load.wait()
        rows = a2d[g]
        gate = jnp.dot(rows, wg[...], preferred_element_type=F32)
        up = jnp.dot(rows, wu[...], preferred_element_type=F32)
        hid[...] = (gate / (1.0 + jnp.exp(-gate)) * up).astype(BF16)
        n_cols = half // 2
        for n in range(4):
            cols = slice(n * n_cols, (n + 1) * n_cols)
            res = lax.dot_general(
                hid[...], wd[cols, :], (((1,), (1,)), ((), ())), preferred_element_type=F32
            )
            own[g, :, cols] = res[0:gr]
            to_left, to_right = res[gr : 2 * gr], res[2 * gr : 3 * gr]
            in_half = slice((n % 2) * n_cols, (n % 2 + 1) * n_cols)
            if n < 2:
                part[g, 0, :, cols] = to_left.astype(BF16)
                pf[g, 1, :, in_half] = to_right
            else:
                pf[g, 0, :, in_half] = to_left
                part[g, 1, :, cols] = to_right.astype(BF16)
            part[g, 2, :, cols] = res[3 * gr : 4 * gr].astype(BF16)
        push(part.at[g, 2, :, lo], rs1.at[g, 0], rs_send.at[g, 0], rs_recv.at[g, 0], right)
        push(part.at[g, 2, :, hi], rs1.at[g, 1], rs_send.at[g, 1], rs_recv.at[g, 1], left)
        push(part.at[g, 1, :, hi], rs2.at[g, 0, :, hi], rs_send.at[g, 2], rs_recv.at[g, 2], right)
        push(part.at[g, 0, :, lo], rs2.at[g, 1, :, lo], rs_send.at[g, 3], rs_recv.at[g, 3], left)

    def s4(g):
        arrive(rs1.at[g, 0], rs_recv.at[g, 0])
        part[g, 1, :, 0:half] = (pf[g, 1] + rs1[g, 0].astype(F32)).astype(BF16)
        push(part.at[g, 1, :, lo], rs2.at[g, 0, :, lo], rs_send.at[g, 4], rs_recv.at[g, 4], right)
        arrive(rs1.at[g, 1], rs_recv.at[g, 1])
        part[g, 0, :, half:width] = (pf[g, 0] + rs1[g, 1].astype(F32)).astype(BF16)
        push(part.at[g, 0, :, hi], rs2.at[g, 1, :, hi], rs_send.at[g, 5], rs_recv.at[g, 5], left)

    def s5(g):
        arrive(rs2.at[g, 0, :, hi], rs_recv.at[g, 2])
        arrive(rs2.at[g, 1, :, lo], rs_recv.at[g, 3])
        arrive(rs2.at[g, 0, :, lo], rs_recv.at[g, 4])
        arrive(rs2.at[g, 1, :, hi], rs_recv.at[g, 5])
        total = own[g] + rs2[g, 0].astype(F32) + rs2[g, 1].astype(F32)
        rows2d[...] = total.astype(BF16)
        to_tiles(ret3, g)
        exchange(ret3, back3, g, -1, back_send, back_recv)

    def s6(g):
        exchanged(back3, g, back_recv)
        from_tiles(back3, g, rows2d)
        rows = rows2d[...]
        res = jnp.dot(whi[g], rows, preferred_element_type=F32)
        res = res + jnp.dot(wlo[g], rows, preferred_element_type=F32)
        acc[...] = acc[...] + res

    def send_counts():
        def one(i, carry):
            pltpu.make_async_remote_copy(
                src_ref=cnt_mine, dst_ref=cnt_all.at[i], send_sem=cnt_send, recv_sem=cnt_recv,
                device_id=relative(1, *split(i)), device_id_type=MESH,
            ).start()
            return carry

        lax.fori_loop(1, plane, one, 0)

    counted = {}

    def plane_counts():
        arrive(cnt_all.at[pl.ds(1, plane - 1)], cnt_recv)
        table = cnt_all[:, 0, :]
        i = lax.broadcasted_iota(I32, (plane, 1), 0)
        sz = (z - lax.shift_right_logical(i, log2(per_z)) + nz) & (nz - 1)
        sy = (y - (lax.shift_right_logical(i, log2(nc)) & (ny - 1)) + ny) & (ny - 1)
        sc = (c - (i & (nc - 1)) + nc) & (nc - 1)
        mine = (z * ny + y) * nc + c
        first = ((sz * ny + sy) * nc + sc < mine).astype(F32)
        counted["inside"] = jnp.sum(table * first, axis=0, keepdims=True)
        tot_mine[...] = jnp.sum(table, axis=0, keepdims=True)
        for k, new_x in enumerate((right, left, opp)):
            push(tot_mine, tot_all.at[k], tot_send.at[k], tot_recv.at[k], new_x)

    def weigh():
        offset = counted["inside"]
        for k, src in enumerate((left, right, opp)):
            arrive(tot_all.at[k], tot_recv.at[k])
            offset = offset + tot_all[k] * jnp.where(src < x, 1.0, 0.0)
        n_experts = cap.shape[1]
        limit = cap[...].astype(F32)
        parts = []
        for k, (oh, rank, pos) in enumerate(((oh0, rank0, pos0), (oh1, rank1, pos1))):
            slot = jnp.sum(oh * offset, axis=1, keepdims=True) + rank
            top = jnp.sum(oh[:, :n_experts] * limit, axis=1, keepdims=True)
            unit = jnp.where(slot < top, units[:, k : k + 1], 0)
            high = unit & ~7
            parts.append((pos, high.astype(F32) / 1024.0, (unit - high).astype(F32) / 1024.0))
        for g in range(len(groups)):
            for k, (pos, high, low) in enumerate(parts):
                here = slots + g * gr == pos
                if k == 0:
                    h, l = jnp.where(here, high, 0.0), jnp.where(here, low, 0.0)
                else:
                    h, l = h + jnp.where(here, high, 0.0), l + jnp.where(here, low, 0.0)
            whi[g] = h.astype(BF16)
            wlo[g] = l.astype(BF16)
        acc[...] = jnp.zeros_like(acc)

    n = len(groups)
    gather(0)
    pl.semaphore_wait(barrier, plane - 1 + nx - 1)
    exchange(out3, recv3, 0, 1, a2a_send, a2a_recv)
    for g in range(1, n):
        gather(g)
        exchange(out3, recv3, g, 1, a2a_send, a2a_recv)
    send_counts()

    if n == 4:
        order = [
            (s1, 0), (s2, 0), (s1, 1), (s3, 0), (s2, 1), (s4, 0), (plane_counts,), (s3, 1), (s1, 2), (s5, 0), (s2, 2), (s4, 1),
            (weigh,), (s1, 3), (s3, 2), (s5, 1), (s2, 3), (s4, 2), (s3, 3), (s5, 2), (s4, 3), (s6, 0), (s6, 1), (s5, 3),
            (s6, 2), (s6, 3),
        ]
    else:
        order = [(stage, g) for stage in (s1, s2, s3, s4, s5) for g in range(n)]
        order += [(plane_counts,), (weigh,)] + [(s6, g) for g in range(n)]
    for stage, *args in order:
        stage(*args)
    out[...] = acc[...].astype(BF16)

    for copy in sent:
        copy.wait_send()
    for g in range(n):
        exchanged(out3, g, a2a_send)
        exchanged(ret3, g, back_send)
    arrive(cnt_all.at[pl.ds(1, plane - 1)], cnt_send)


def local(shape, most, tokens, expert_ids, gate_units, capacity, w_gate, w_up, w_down):
    nx, nz, ny, nc = shape
    t_rows, width = tokens.shape
    ff = w_gate.shape[2]
    plane = nz * ny * nc
    n = len(z_groups(nz))
    gr = 2 * ny * nc * most
    vmem = pl.BlockSpec(memory_space=pltpu.VMEM)
    anywhere = pl.BlockSpec(memory_space=pl.ANY)
    dma = pltpu.SemaphoreType.DMA
    tiles = pltpu.VMEM((plane * most, ROW_TILE, LANES), BF16)
    return pl.pallas_call(
        functools.partial(kernel, shape, most),
        out_shape=jax.ShapeDtypeStruct((t_rows, width), BF16),
        in_specs=[vmem, vmem, vmem, vmem, anywhere, anywhere, anywhere],
        out_specs=vmem,
        scratch_shapes=[
            pltpu.VMEM((width, ff), BF16),
            pltpu.VMEM((width, ff), BF16),
            pltpu.VMEM((width, ff), BF16),
            pltpu.VMEM((256, 256), BF16),
            pltpu.VMEM((gr, width), BF16),
            tiles, tiles, tiles, tiles,
            pltpu.VMEM((n, nx * gr, width), BF16),
            pltpu.VMEM((nx * gr, ff), BF16),
            pltpu.VMEM((n, gr, width), F32),
            pltpu.VMEM((n, 2, gr, width // 2), F32),
            pltpu.VMEM((n, 3, gr, width), BF16),
            pltpu.VMEM((n, 2, gr, width // 2), BF16),
            pltpu.VMEM((n, 2, gr, width), BF16),
            pltpu.VMEM((8, LANES), F32),
            pltpu.VMEM((n, t_rows, gr), BF16),
            pltpu.VMEM((n, t_rows, gr), BF16),
            pltpu.VMEM((t_rows, width), F32),
            pltpu.VMEM((1, LANES), F32),
            pltpu.VMEM((plane, 1, LANES), F32),
            pltpu.VMEM((1, LANES), F32),
            pltpu.VMEM((3, 1, LANES), F32),
            dma((3,)),
            dma((n,)), dma((n,)),
            dma((n, 6)), dma((n, 6)),
            dma((n, 6)), dma((n, 6)),
            dma((n,)), dma((n,)),
            dma, dma,
            dma((3,)), dma((3,)),
        ],
        compiler_params=pltpu.CompilerParams(collective_id=0, has_side_effects=True),
    )(tokens, expert_ids, gate_units, capacity.reshape(1, -1), w_gate, w_up, w_down)


def build(finer, most):
    shape = tuple(finer.shape[a] for a in AXES)
    return jax.shard_map(
        functools.partial(local, shape, most),
        mesh=finer,
        in_specs=(
            P(AXES, None),
            P(AXES, None),
            P(AXES, None),
            P(),
            P(EXPERT, None, "dp"),
            P(EXPERT, None, "dp"),
            P(EXPERT, None, "dp"),
        ),
        out_specs=P(AXES, None),
        check_vma=False,
    )


def solution(mesh):
    finer = Mesh(mesh.devices.reshape(mesh.shape["dp"], 8, 4, 2), AXES)
    return build(finer, 5)
```

```python
import functools

import jax
import jax.numpy as jnp
from jax import lax
from jax.experimental import pallas as pl
from jax.experimental.pallas import tpu as pltpu
from jax.sharding import Mesh
from jax.sharding import PartitionSpec as P

MESH = pl.DeviceIdType.MESH
AXES = ("dp", "expert_0", "expert_1", "expert_2")
EXPERT = ("expert_0", "expert_1", "expert_2")
BF16, F32, I32 = jnp.bfloat16, jnp.float32, jnp.int32
LANES = 128
ROW_TILE = 16


def offset_groups(nz, ny):
    if (nz, ny) != (8, 4):
        first = [(dz, dy) for dz in (0, 1) for dy in range(ny)]
        return [first] + [
            [(dz, dy) for dz in (-k, k + 1) for dy in range(ny)] for k in reversed(range(1, nz // 2))
        ]
    return [
        [(0, 0), (0, 1), (0, 2), (0, 3), (1, 0), (-1, 0), (1, 3), (-1, 3)],
        [(-2, 2), (-2, 3), (3, 0), (3, 1), (-3, 0), (-3, 1), (4, 0), (4, 1)],
        [(2, 2), (2, 3), (3, 2), (3, 3), (-3, 2), (-3, 3), (4, 2), (4, 3)],
        [(1, 1), (-1, 1), (1, 2), (-1, 2), (2, 0), (-2, 0), (2, 1), (-2, 1)],
    ]


def log2(n):
    assert n & (n - 1) == 0
    return n.bit_length() - 1


def kernel(
    shape, most,
    tokens_h, ids_h, units_h, cap_h, wg_h, wu_h, wd_h, out,
    tokens, ids, units, cap, wg, wu, wd, perm, rows2d, out3, recv3, ret3, back3, a2d, hid, own, pf, part, rs1, rs2,
    sel, whi, wlo, acc, cnt_mine, cnt_all, tot_mine, tot_all,
    near, w_sem, a2a_send, a2a_recv, ag_send, ag_recv, rs_send, rs_recv, back_send, back_recv, cnt_send, cnt_recv, tot_send, tot_recv,
):
    nx, nz, ny, nc = shape
    x, z, y, c = (lax.axis_index(a) for a in AXES)
    right, left, opp = lax.rem(x + 1, nx), lax.rem(x + nx - 1, nx), lax.rem(x + 2, nx)
    plane = nz * ny * nc
    per_z = ny * nc
    groups = offset_groups(nz, ny)
    per_group = len(groups[0]) * nc
    gr = per_group * most
    blocks = gr // ROW_TILE
    t_rows, width = tokens.shape
    half = width // 2
    lo, hi = pl.ds(0, half), pl.ds(half, half)

    def at_x(new_x):
        return (new_x, z, y, c)

    def relative(sign, dz, dy, dc):
        return (
            x,
            lax.rem(z + sign * dz + 2 * nz, nz),
            lax.rem(y + sign * dy + ny, ny),
            lax.rem(c + sign * dc + nc, nc),
        )

    def split(i):
        return i // per_z, lax.rem(i // nc, ny), lax.rem(i, nc)

    barrier = pltpu.get_barrier_semaphore()
    nearby = min(3, nz) * per_z

    def greet(i, carry):
        dz, dy, dc = split(i)
        dz = jnp.where(dz == 2, -1, dz)
        pl.semaphore_signal(barrier, inc=1, device_id=relative(1, dz, dy, dc), device_id_type=MESH)
        return carry

    for new_x in (right, left, opp):
        pl.semaphore_signal(barrier, inc=1, device_id=at_x(new_x), device_id_type=MESH)
    lax.fori_loop(1, nearby, greet, 0)

    small = [
        pltpu.make_async_copy(src, dst, w_sem.at[i])
        for i, (src, dst) in enumerate(((ids_h, ids), (tokens_h, tokens), (units_h, units), (cap_h, cap)))
    ]
    loads = [
        pltpu.make_async_copy(src.at[0], dst, w_sem.at[4 + i])
        for i, (src, dst) in enumerate(((wg_h, wg), (wu_h, wu), (wd_h, wd)))
    ]
    for load in small + loads:
        load.start()

    def near_ready():
        pl.semaphore_wait(barrier, nearby - 1 + nx - 1)

    def tell(step):
        for dz in (1, -1):
            pl.semaphore_signal(near.at[step], inc=1, device_id=relative(1, dz, 0, 0), device_id_type=MESH)

    def told(step):
        pl.semaphore_wait(near.at[step], 2)

    i_row = lax.broadcasted_iota(I32, (256, 256), 0)
    i_col = lax.broadcasted_iota(I32, (256, 256), 1)
    swapped = (i_row & 15) * 16 + lax.shift_right_logical(i_row, 4)
    perm[...] = (i_col == swapped).astype(BF16)
    small[0].wait()

    n_experts = cap.shape[1]
    expert = lax.broadcasted_iota(I32, (n_experts, t_rows), 0)
    id0, id1 = ids[0:1, :], ids[1:2, :]
    oh0, oh1 = (expert == id0).astype(F32), (expert == id1).astype(F32)
    named = (oh0 + oh1).astype(BF16)
    counts = lax.dot_general(
        jnp.ones((8, t_rows), BF16), named, (((1,), (1,)), ((), ())), preferred_element_type=F32
    )[0:1, :]
    cnt_mine[:, 0:n_experts] = counts
    cnt_all[0, :, 0:n_experts] = counts
    earlier = (
        lax.broadcasted_iota(I32, (t_rows, t_rows), 0) < lax.broadcasted_iota(I32, (t_rows, t_rows), 1)
    ).astype(BF16)
    before = jnp.dot(named, earlier, preferred_element_type=F32)
    rank0 = jnp.sum(before * oh0, axis=0, keepdims=True)
    rank1 = jnp.sum(before * oh1, axis=0, keepdims=True)

    def slot_of(expert, rank):
        ez = lax.shift_right_logical(expert, log2(per_z))
        ey = lax.shift_right_logical(expert, log2(nc)) & (ny - 1)
        ec = expert & (nc - 1)
        dz = (ez - z + nz) & (nz - 1)
        dy = (ey - y + ny) & (ny - 1)
        dc = (ec - c + nc) & (nc - 1)
        key, place = dz * ny + dy, jnp.zeros_like(dz)
        for i, (z_off, y_off) in enumerate(pair for group in groups for pair in group):
            place = jnp.where(key == (z_off % nz) * ny + y_off, i, place)
        return (place * nc + dc) * most + rank.astype(I32)

    pos0, pos1 = slot_of(id0, rank0), slot_of(id1, rank1)
    small[1].wait()

    def to_tiles(dst3, g):
        for b in range(blocks):
            block = rows2d[ROW_TILE * b : ROW_TILE * (b + 1), :]
            stacked = jnp.concatenate(
                [block[:, LANES * s : LANES * (s + 1)] for s in range(width // LANES)], axis=0
            )
            turned = jnp.dot(perm[...], stacked, preferred_element_type=F32).astype(BF16)
            r = g * gr + ROW_TILE * b
            dst3[r : r + ROW_TILE] = turned.reshape(ROW_TILE, ROW_TILE, LANES)

    def from_tiles(src3, g, dst):
        for b in range(blocks):
            r = g * gr + ROW_TILE * b
            stacked = src3[r : r + ROW_TILE].reshape(ROW_TILE * ROW_TILE, LANES)
            turned = jnp.dot(perm[...], stacked, preferred_element_type=F32).astype(BF16)
            for s in range(width // LANES):
                dst[ROW_TILE * b : ROW_TILE * (b + 1), LANES * s : LANES * (s + 1)] = turned[
                    ROW_TILE * s : ROW_TILE * (s + 1), :
                ]

    def exchange(src, dst, g, sign, send_sem, recv_sem):
        base = g * per_group
        for i, (dz, dy) in enumerate(groups[g]):
            for dc in range(nc):
                rows = pl.ds((base + i * nc + dc) * most, most)
                if dz == dy == dc == 0:
                    assert i == 0
                    continue
                pltpu.make_async_remote_copy(
                    src_ref=src.at[rows],
                    dst_ref=dst.at[rows],
                    send_sem=send_sem.at[g],
                    recv_sem=recv_sem.at[g],
                    device_id=relative(1, sign * dz, sign * dy, sign * dc),
                    device_id_type=MESH,
                ).start()
        if groups[g][0] == (0, 0):
            dst[base * most : (base + 1) * most] = src[base * most : (base + 1) * most]

    def exchanged(ref, g, sem):
        first = 1 if groups[g][0] == (0, 0) else 0
        rows = pl.ds((g * per_group + first) * most, (per_group - first) * most)
        with jax.named_scope("wait"):
            pltpu.make_async_copy(ref.at[rows], ref.at[rows], sem.at[g]).wait()

    slots = lax.broadcasted_iota(I32, (gr, t_rows), 0)

    def gather(g):
        s0, s1 = (slots + g * gr == pos0), (slots + g * gr == pos1)
        chosen = (s0.astype(F32) + s1.astype(F32)).astype(BF16)
        rows = jnp.dot(chosen, tokens[...], preferred_element_type=F32)
        rows2d[...] = rows.astype(BF16)
        to_tiles(out3, g)

    sent = []

    def push(src, dst, send_sem, recv_sem, new_x):
        copy = pltpu.make_async_remote_copy(
            src_ref=src, dst_ref=dst, send_sem=send_sem, recv_sem=recv_sem,
            device_id=at_x(new_x), device_id_type=MESH,
        )
        copy.start()
        sent.append(copy)

    def arrive(ref, sem):
        with jax.named_scope("wait"):
            pltpu.make_async_copy(ref, ref, sem).wait()

    def rows_of(slot):
        return pl.ds(slot * gr, gr)

    def s1(g):
        exchanged(recv3, g, a2a_recv)
        from_tiles(recv3, g, a2d.at[g])
        me = rows_of(0)
        push(a2d.at[g, me, lo], a2d.at[g, rows_of(1), lo], ag_send.at[g, 0], ag_recv.at[g, 0], right)
        push(a2d.at[g, me, hi], a2d.at[g, rows_of(2), hi], ag_send.at[g, 1], ag_recv.at[g, 1], left)
        push(a2d.at[g, me, hi], a2d.at[g, rows_of(1), hi], ag_send.at[g, 2], ag_recv.at[g, 2], right)
        push(a2d.at[g, me, lo], a2d.at[g, rows_of(2), lo], ag_send.at[g, 3], ag_recv.at[g, 3], left)

    def s2(g):
        arrive(a2d.at[g, rows_of(1), lo], ag_recv.at[g, 0])
        push(a2d.at[g, rows_of(1), lo], a2d.at[g, rows_of(3), lo], ag_send.at[g, 4], ag_recv.at[g, 4], right)
        arrive(a2d.at[g, rows_of(2), hi], ag_recv.at[g, 1])
        push(a2d.at[g, rows_of(2), hi], a2d.at[g, rows_of(3), hi], ag_send.at[g, 5], ag_recv.at[g, 5], left)

    def s3(g):
        arrive(a2d.at[g, rows_of(1), hi], ag_recv.at[g, 2])
        arrive(a2d.at[g, rows_of(2), lo], ag_recv.at[g, 3])
        arrive(a2d.at[g, rows_of(3), lo], ag_recv.at[g, 4])
        arrive(a2d.at[g, rows_of(3), hi], ag_recv.at[g, 5])
        while loads:
            loads.pop().wait()
        rows = a2d[g]
        by_unit = (((1,), (1,)), ((), ()))
        gate = lax.dot_general(rows, wg[...], by_unit, preferred_element_type=F32)
        up = lax.dot_general(rows, wu[...], by_unit, preferred_element_type=F32)
        hid[...] = (gate / (1.0 + jnp.exp(-gate)) * up).astype(BF16)
        n_cols = half // 2
        for n in range(4):
            cols = slice(n * n_cols, (n + 1) * n_cols)
            res = jnp.dot(hid[...], wd[:, cols], preferred_element_type=F32)
            own[g, :, cols] = res[0:gr]
            to_left, to_right = res[gr : 2 * gr], res[2 * gr : 3 * gr]
            in_half = slice((n % 2) * n_cols, (n % 2 + 1) * n_cols)
            if n < 2:
                part[g, 0, :, cols] = to_left.astype(BF16)
                pf[g, 1, :, in_half] = to_right
            else:
                pf[g, 0, :, in_half] = to_left
                part[g, 1, :, cols] = to_right.astype(BF16)
            part[g, 2, :, cols] = res[3 * gr : 4 * gr].astype(BF16)
        push(part.at[g, 2, :, lo], rs1.at[g, 0], rs_send.at[g, 0], rs_recv.at[g, 0], right)
        push(part.at[g, 2, :, hi], rs1.at[g, 1], rs_send.at[g, 1], rs_recv.at[g, 1], left)
        push(part.at[g, 1, :, hi], rs2.at[g, 0, :, hi], rs_send.at[g, 2], rs_recv.at[g, 2], right)
        push(part.at[g, 0, :, lo], rs2.at[g, 1, :, lo], rs_send.at[g, 3], rs_recv.at[g, 3], left)

    def s4(g):
        arrive(rs1.at[g, 0], rs_recv.at[g, 0])
        part[g, 1, :, 0:half] = (pf[g, 1] + rs1[g, 0].astype(F32)).astype(BF16)
        push(part.at[g, 1, :, lo], rs2.at[g, 0, :, lo], rs_send.at[g, 4], rs_recv.at[g, 4], right)
        arrive(rs1.at[g, 1], rs_recv.at[g, 1])
        part[g, 0, :, half:width] = (pf[g, 0] + rs1[g, 1].astype(F32)).astype(BF16)
        push(part.at[g, 0, :, hi], rs2.at[g, 1, :, hi], rs_send.at[g, 5], rs_recv.at[g, 5], left)

    def s5(g):
        arrive(rs2.at[g, 0, :, hi], rs_recv.at[g, 2])
        arrive(rs2.at[g, 1, :, lo], rs_recv.at[g, 3])
        arrive(rs2.at[g, 0, :, lo], rs_recv.at[g, 4])
        arrive(rs2.at[g, 1, :, hi], rs_recv.at[g, 5])
        total = own[g] + rs2[g, 0].astype(F32) + rs2[g, 1].astype(F32)
        rows2d[...] = total.astype(BF16)
        to_tiles(ret3, g)
        exchange(ret3, back3, g, -1, back_send, back_recv)

    def s6(g):
        exchanged(back3, g, back_recv)
        from_tiles(back3, g, rows2d)
        rows = rows2d[...]
        res = jnp.dot(whi[g], rows, preferred_element_type=F32)
        res = res + jnp.dot(wlo[g], rows, preferred_element_type=F32)
        acc[...] = acc[...] + res

    def send_counts():
        def one(i, carry):
            pltpu.make_async_remote_copy(
                src_ref=cnt_mine, dst_ref=cnt_all.at[i], send_sem=cnt_send, recv_sem=cnt_recv,
                device_id=relative(1, *split(i)), device_id_type=MESH,
            ).start()
            return carry

        lax.fori_loop(1, plane, one, 0)

    counted = {}

    def plane_counts():
        arrive(cnt_all.at[pl.ds(1, plane - 1)], cnt_recv)
        table = cnt_all[:, 0, 0:n_experts]
        i = lax.broadcasted_iota(I32, (plane, 1), 0)
        sz = (z - lax.shift_right_logical(i, log2(per_z)) + nz) & (nz - 1)
        sy = (y - (lax.shift_right_logical(i, log2(nc)) & (ny - 1)) + ny) & (ny - 1)
        sc = (c - (i & (nc - 1)) + nc) & (nc - 1)
        mine = (z * ny + y) * nc + c
        first = ((sz * ny + sy) * nc + sc < mine).astype(F32)
        counted["inside"] = jnp.sum(table * first, axis=0, keepdims=True)
        tot_mine[:, 0:n_experts] = jnp.sum(table, axis=0, keepdims=True)
        for k, new_x in enumerate((right, left, opp)):
            push(tot_mine, tot_all.at[k], tot_send.at[k], tot_recv.at[k], new_x)

    def weigh():
        small[2].wait()
        small[3].wait()
        offset = counted["inside"]
        for k, src in enumerate((left, right, opp)):
            arrive(tot_all.at[k], tot_recv.at[k])
            offset = offset + tot_all[k][:, 0:n_experts] * jnp.where(src < x, 1.0, 0.0)
        diagonal = lax.broadcasted_iota(I32, (n_experts, n_experts), 0) == lax.broadcasted_iota(
            I32, (n_experts, n_experts), 1
        )

        def down(row):
            return jnp.sum(jnp.where(diagonal, row, 0.0), axis=1, keepdims=True)

        offset, limit = down(offset), down(cap[...].astype(F32))
        parts = []
        for k, (oh, rank, pos) in enumerate(((oh0, rank0, pos0), (oh1, rank1, pos1))):
            slot = jnp.sum(oh * offset, axis=0, keepdims=True) + rank
            top = jnp.sum(oh * limit, axis=0, keepdims=True)
            unit = jnp.where(slot < top, units[k : k + 1, :], 0)
            high = unit & ~7
            parts.append((pos, high.astype(F32) / 1024.0, (unit - high).astype(F32) / 1024.0))
        wide = lax.broadcasted_iota(I32, (LANES, t_rows), 0)
        for g in range(len(groups)):
            h = l = jnp.zeros((LANES, t_rows), F32)
            for pos, high, low in parts:
                here = wide + g * gr == pos
                h, l = h + jnp.where(here, high, 0.0), l + jnp.where(here, low, 0.0)
            whi[g] = jnp.transpose(h)[:, 0:gr].astype(BF16)
            wlo[g] = jnp.transpose(l)[:, 0:gr].astype(BF16)
        acc[...] = jnp.zeros_like(acc)

    n = len(groups)
    issue = [0, 3, 1, 2] if n == 4 else list(range(n))
    with jax.named_scope("gather_0"):
        gather(0)
    with jax.named_scope("barrier"):
        near_ready()
        tell(0)
    with jax.named_scope("send_0"):
        exchange(out3, recv3, 0, 1, a2a_send, a2a_recv)
    steps = nz // 2 - 1
    for step in range(steps):
        with jax.named_scope("told"):
            told(step)
            if step + 1 < steps:
                tell(step + 1)
        if step == 0:
            with jax.named_scope("gather"):
                gather(issue[1])
    for g in issue[1:]:
        if g != issue[1]:
            with jax.named_scope("gather"):
                gather(g)
        with jax.named_scope("send"):
            exchange(out3, recv3, g, 1, a2a_send, a2a_recv)

    if n == 4:
        order = [
            (s1, 0), (s1, 3), (s2, 0), (s2, 3), (send_counts,), (s1, 1), (s3, 3), (s2, 1), (s1, 2), (s4, 3), (s3, 1), (s4, 1),
            (s5, 3), (s2, 2), (plane_counts,), (s5, 1), (s3, 2), (s4, 2), (s3, 0), (weigh,), (s5, 2), (s4, 0),
            (s6, 3), (s6, 1), (s5, 0), (s6, 2), (s6, 0),
        ]
    else:
        order = [(stage, g) for stage in (s1, s2, s3, s4, s5) for g in range(n)]
        order += [(send_counts,), (plane_counts,), (weigh,)] + [(s6, g) for g in range(n)]
    for stage, *args in order:
        with jax.named_scope("_".join([stage.__name__, *map(str, args)])):
            stage(*args)
    out[...] = acc[...].astype(BF16)

    for copy in sent:
        copy.wait_send()
    for g in range(n):
        exchanged(out3, g, a2a_send)
        exchanged(ret3, g, back_send)
    arrive(cnt_all.at[pl.ds(1, plane - 1)], cnt_send)


def local(shape, most, tokens, expert_ids, gate_units, capacity, w_gate, w_up, w_down):
    nx, nz, ny, nc = shape
    t_rows, width = tokens.shape
    ff = w_gate.shape[2]
    turn = functools.partial(jnp.swapaxes, axis1=-1, axis2=-2)
    plane = nz * ny * nc
    groups = offset_groups(nz, ny)
    n, gr = len(groups), len(groups[0]) * nc * most
    vmem = pl.BlockSpec(memory_space=pltpu.VMEM)
    anywhere = pl.BlockSpec(memory_space=pl.ANY)
    dma = pltpu.SemaphoreType.DMA
    tiles = pltpu.VMEM((plane * most, ROW_TILE, LANES), BF16)
    return pl.pallas_call(
        functools.partial(kernel, shape, most),
        out_shape=jax.ShapeDtypeStruct((t_rows, width), BF16),
        in_specs=[anywhere] * 7,
        out_specs=vmem,
        scratch_shapes=[
            pltpu.VMEM((t_rows, width), BF16),
            pltpu.VMEM((2, t_rows), I32),
            pltpu.VMEM((2, t_rows), I32),
            pltpu.VMEM((1, plane), I32),
            pltpu.VMEM((ff, width), BF16),
            pltpu.VMEM((ff, width), BF16),
            pltpu.VMEM((ff, width), BF16),
            pltpu.VMEM((256, 256), BF16),
            pltpu.VMEM((gr, width), BF16),
            tiles, tiles, tiles, tiles,
            pltpu.VMEM((n, nx * gr, width), BF16),
            pltpu.VMEM((nx * gr, ff), BF16),
            pltpu.VMEM((n, gr, width), F32),
            pltpu.VMEM((n, 2, gr, width // 2), F32),
            pltpu.VMEM((n, 3, gr, width), BF16),
            pltpu.VMEM((n, 2, gr, width // 2), BF16),
            pltpu.VMEM((n, 2, gr, width), BF16),
            pltpu.VMEM((8, LANES), F32),
            pltpu.VMEM((n, t_rows, gr), BF16),
            pltpu.VMEM((n, t_rows, gr), BF16),
            pltpu.VMEM((t_rows, width), F32),
            pltpu.VMEM((1, LANES), F32),
            pltpu.VMEM((plane, 1, LANES), F32),
            pltpu.VMEM((1, LANES), F32),
            pltpu.VMEM((3, 1, LANES), F32),
            pltpu.SemaphoreType.REGULAR((nz // 2 - 1,)),
            dma((7,)),
            dma((n,)), dma((n,)),
            dma((n, 6)), dma((n, 6)),
            dma((n, 6)), dma((n, 6)),
            dma((n,)), dma((n,)),
            dma, dma,
            dma((3,)), dma((3,)),
        ],
        compiler_params=pltpu.CompilerParams(collective_id=0, has_side_effects=True),
    )(tokens, turn(expert_ids), turn(gate_units), capacity.reshape(1, -1), turn(w_gate), turn(w_up), turn(w_down))


def build(finer, most):
    shape = tuple(finer.shape[a] for a in AXES)
    return jax.shard_map(
        functools.partial(local, shape, most),
        mesh=finer,
        in_specs=(
            P(AXES, None),
            P(AXES, None),
            P(AXES, None),
            P(),
            P(EXPERT, None, "dp"),
            P(EXPERT, None, "dp"),
            P(EXPERT, None, "dp"),
        ),
        out_specs=P(AXES, None),
        check_vma=False,
    )


def solution(mesh):
    finer = Mesh(mesh.devices.reshape(mesh.shape["dp"], 8, 4, 2), AXES)
    return build(finer, 5)
```

```python
import functools

import jax
import jax.numpy as jnp
from jax import lax
from jax.experimental import pallas as pl
from jax.experimental.pallas import tpu as pltpu
from jax.sharding import Mesh
from jax.sharding import PartitionSpec as P

MESH = pl.DeviceIdType.MESH
AXES = ("dp", "expert_0", "expert_1", "expert_2")
EXPERT = ("expert_0", "expert_1", "expert_2")
BF16, F32, I32 = jnp.bfloat16, jnp.float32, jnp.int32
LANES = 128
ROW_TILE = 16


def offset_groups(nz, ny):
    if (nz, ny) != (8, 4):
        first = [(dz, dy) for dz in (0, 1) for dy in range(ny)]
        return [first] + [
            [(dz, dy) for dz in (k + 1, -k) for dy in range(ny)] for k in reversed(range(1, nz // 2))
        ]
    return [
        [(0, 0), (0, 1), (0, 2), (0, 3), (1, 0), (-1, 0), (1, 3), (-1, 3)],
        [(-2, 2), (-2, 3), (2, 2), (2, 3), (3, 0), (-3, 0), (3, 1), (-3, 1)],
        [(4, 0), (4, 1), (3, 2), (3, 3), (-3, 2), (-3, 3), (4, 2), (4, 3)],
        [(1, 1), (-1, 1), (1, 2), (-1, 2), (2, 0), (-2, 0), (2, 1), (-2, 1)],
    ]


def log2(n):
    assert n & (n - 1) == 0
    return n.bit_length() - 1


def kernel(
    shape, most,
    tokens_h, ids_h, units_h, cap_h, wg_h, wu_h, wd_h, out,
    tokens, ids, units, cap, wg, wu, wd, perm, rows2d, out3, recv3, ret3, back3, a2d, hid, own, pf, part, rs1, rs2,
    sel, whi, wlo, acc, cnt_mine, cnt_all, tot_mine, tot_all,
    fx, fr, fs, fb, f1, f2, fsum, relayed,
    near, w_sem, a2a_send, a2a_recv, ag_send, ag_recv, rs_send, rs_recv, back_send, back_recv, cnt_send, cnt_recv, tot_send, tot_recv,
    fx_send, fx_recv, fb_send, fb_recv, relay_send, relay_recv,
):
    nx, nz, ny, nc = shape
    x, z, y, c = (lax.axis_index(a) for a in AXES)
    right, left, opp = lax.rem(x + 1, nx), lax.rem(x + nx - 1, nx), lax.rem(x + 2, nx)
    plane = nz * ny * nc
    per_z = ny * nc
    groups = offset_groups(nz, ny)
    per_group = len(groups[0]) * nc
    far = [g for g, group in enumerate(groups) if group[0][0] == nz // 2 > 1]
    far_offsets = min(2, ny)
    gr = per_group * most
    blocks = gr // ROW_TILE
    t_rows, width = tokens.shape
    half = width // 2
    lo, hi = pl.ds(0, half), pl.ds(half, half)

    def at_x(new_x):
        return (new_x, z, y, c)

    def relative(sign, dz, dy, dc):
        return (
            x,
            lax.rem(z + sign * dz + 2 * nz, nz),
            lax.rem(y + sign * dy + ny, ny),
            lax.rem(c + sign * dc + nc, nc),
        )

    def split(i):
        return i // per_z, lax.rem(i // nc, ny), lax.rem(i, nc)

    barrier = pltpu.get_barrier_semaphore()
    nearby = min(3, nz) * per_z

    def greet(i, carry):
        dz, dy, dc = split(i)
        dz = jnp.where(dz == 2, -1, dz)
        pl.semaphore_signal(barrier, inc=1, device_id=relative(1, dz, dy, dc), device_id_type=MESH)
        return carry

    for new_x in (right, left, opp):
        pl.semaphore_signal(barrier, inc=1, device_id=at_x(new_x), device_id_type=MESH)
    lax.fori_loop(1, nearby, greet, 0)

    small = [
        pltpu.make_async_copy(src, dst, w_sem.at[i])
        for i, (src, dst) in enumerate(((ids_h, ids), (tokens_h, tokens), (units_h, units), (cap_h, cap)))
    ]
    loads = [
        pltpu.make_async_copy(src.at[0], dst, w_sem.at[4 + i])
        for i, (src, dst) in enumerate(((wg_h, wg), (wu_h, wu), (wd_h, wd)))
    ]
    for load in small + loads:
        load.start()

    def near_ready():
        pl.semaphore_wait(barrier, nearby - 1 + nx - 1)

    def tell(step):
        for dz in (1, -1):
            pl.semaphore_signal(near.at[step], inc=1, device_id=relative(1, dz, 0, 0), device_id_type=MESH)

    def told(step):
        pl.semaphore_wait(near.at[step], 2)

    i_row = lax.broadcasted_iota(I32, (256, 256), 0)
    i_col = lax.broadcasted_iota(I32, (256, 256), 1)
    swapped = (i_row & 15) * 16 + lax.shift_right_logical(i_row, 4)
    perm[...] = (i_col == swapped).astype(BF16)
    small[0].wait()

    n_experts = cap.shape[1]
    expert = lax.broadcasted_iota(I32, (n_experts, t_rows), 0)
    id0, id1 = ids[0:1, :], ids[1:2, :]
    oh0, oh1 = (expert == id0).astype(F32), (expert == id1).astype(F32)
    named = (oh0 + oh1).astype(BF16)
    counts = lax.dot_general(
        jnp.ones((8, t_rows), BF16), named, (((1,), (1,)), ((), ())), preferred_element_type=F32
    )[0:1, :]
    cnt_mine[:, 0:n_experts] = counts
    cnt_all[0, :, 0:n_experts] = counts
    earlier = (
        lax.broadcasted_iota(I32, (t_rows, t_rows), 0) < lax.broadcasted_iota(I32, (t_rows, t_rows), 1)
    ).astype(BF16)
    before = jnp.dot(named, earlier, preferred_element_type=F32)
    rank0 = jnp.sum(before * oh0, axis=0, keepdims=True)
    rank1 = jnp.sum(before * oh1, axis=0, keepdims=True)

    def slot_of(expert, rank):
        ez = lax.shift_right_logical(expert, log2(per_z))
        ey = lax.shift_right_logical(expert, log2(nc)) & (ny - 1)
        ec = expert & (nc - 1)
        dz = (ez - z + nz) & (nz - 1)
        dy = (ey - y + ny) & (ny - 1)
        dc = (ec - c + nc) & (nc - 1)
        key, place = dz * ny + dy, jnp.zeros_like(dz)
        for i, (z_off, y_off) in enumerate(pair for group in groups for pair in group):
            place = jnp.where(key == (z_off % nz) * ny + y_off, i, place)
        return (place * nc + dc) * most + rank.astype(I32)

    pos0, pos1 = slot_of(id0, rank0), slot_of(id1, rank1)
    small[1].wait()

    def to_tiles(src, dst3, r0):
        for b in range(blocks):
            block = src[ROW_TILE * b : ROW_TILE * (b + 1), :]
            stacked = jnp.concatenate(
                [block[:, LANES * s : LANES * (s + 1)] for s in range(width // LANES)], axis=0
            )
            turned = jnp.dot(perm[...], stacked, preferred_element_type=F32).astype(BF16)
            r = r0 + ROW_TILE * b
            dst3[r : r + ROW_TILE] = turned.reshape(ROW_TILE, ROW_TILE, LANES)

    def from_tiles(block_of, dst):
        for b in range(blocks):
            stacked = block_of(ROW_TILE * b).reshape(ROW_TILE * ROW_TILE, LANES)
            turned = jnp.dot(perm[...], stacked, preferred_element_type=F32).astype(BF16)
            for s in range(width // LANES):
                dst[ROW_TILE * b : ROW_TILE * (b + 1), LANES * s : LANES * (s + 1)] = turned[
                    ROW_TILE * s : ROW_TILE * (s + 1), :
                ]

    def block_in(src3, r0):
        return lambda r: src3[r0 + r : r0 + r + ROW_TILE]

    def exchange(src, dst, g, sign, send_sem, recv_sem):
        base = g * per_group if g else 0
        for i, (dz, dy) in enumerate(groups[g]):
            for dc in range(nc):
                rows = pl.ds((base + i * nc + dc) * most, most)
                rows = rows if g else (slice(None), rows)
                if dz == dy == dc == 0:
                    assert i == 0
                    continue
                target, arrival, z_off = dst.at[rows], recv_sem.at[g], sign * dz
                if g in far and i < far_offsets:
                    way = 0 if sign == 1 else 1
                    target = relayed.at[way, pl.ds((i * nc + dc) * most, most)]
                    arrival, z_off = relay_recv.at[way], -(nz // 4)
                pltpu.make_async_remote_copy(
                    src_ref=src.at[rows],
                    dst_ref=target,
                    send_sem=send_sem.at[g],
                    recv_sem=arrival,
                    device_id=relative(1, z_off, sign * dy, sign * dc),
                    device_id_type=MESH,
                ).start()
        if g == 0:
            dst[:, 0:most] = src[:, 0:most]

    def exchanged(ref, g, sem):
        rows = pl.ds(g * per_group * most, per_group * most)
        if g == 0:
            rows = (slice(None), pl.ds(most, (per_group - 1) * most))
        with jax.named_scope("wait"):
            pltpu.make_async_copy(ref.at[rows], ref.at[rows], sem.at[g]).wait()

    slots = lax.broadcasted_iota(I32, (gr, t_rows), 0)

    def gather(g):
        s0, s1 = (slots + g * gr == pos0), (slots + g * gr == pos1)
        chosen = (s0.astype(F32) + s1.astype(F32)).astype(BF16)
        rows = jnp.dot(chosen, tokens[...], preferred_element_type=F32)
        rows2d[...] = rows.astype(BF16)
        if g:
            to_tiles(rows2d, out3, g * gr)
        else:
            to_tiles(rows2d, fx.at[0], 0)

    sent = []

    def push(src, dst, send_sem, recv_sem, new_x):
        copy = pltpu.make_async_remote_copy(
            src_ref=src, dst_ref=dst, send_sem=send_sem, recv_sem=recv_sem,
            device_id=at_x(new_x), device_id_type=MESH,
        )
        copy.start()
        sent.append(copy)

    def arrive(ref, sem):
        with jax.named_scope("wait"):
            pltpu.make_async_copy(ref, ref, sem).wait()

    def rows_of(slot):
        return pl.ds(slot * gr, gr)

    def onward(way):
        (g,) = far
        rows = pl.ds(g * per_group * most, far_offsets * nc * most)
        dst, recv_sem = ((recv3, a2a_recv), (back3, back_recv))[way]
        arrive(relayed.at[way], relay_recv.at[way])
        copy = pltpu.make_async_remote_copy(
            src_ref=relayed.at[way], dst_ref=dst.at[rows], send_sem=relay_send.at[way], recv_sem=recv_sem.at[g],
            device_id=relative(1, -(nz // 4), 0, 0), device_id_type=MESH,
        )
        copy.start()
        sent.append(copy)

    def s1(g):
        exchanged(recv3, g, a2a_recv)
        from_tiles(block_in(recv3, g * gr), a2d.at[g])
        me = rows_of(0)
        push(a2d.at[g, me, lo], a2d.at[g, rows_of(1), lo], ag_send.at[g, 0], ag_recv.at[g, 0], right)
        push(a2d.at[g, me, hi], a2d.at[g, rows_of(2), hi], ag_send.at[g, 1], ag_recv.at[g, 1], left)
        push(a2d.at[g, me, hi], a2d.at[g, rows_of(1), hi], ag_send.at[g, 2], ag_recv.at[g, 2], right)
        push(a2d.at[g, me, lo], a2d.at[g, rows_of(2), lo], ag_send.at[g, 3], ag_recv.at[g, 3], left)

    def s2(g):
        arrive(a2d.at[g, rows_of(1), lo], ag_recv.at[g, 0])
        push(a2d.at[g, rows_of(1), lo], a2d.at[g, rows_of(3), lo], ag_send.at[g, 4], ag_recv.at[g, 4], right)
        arrive(a2d.at[g, rows_of(2), hi], ag_recv.at[g, 1])
        push(a2d.at[g, rows_of(2), hi], a2d.at[g, rows_of(3), hi], ag_send.at[g, 5], ag_recv.at[g, 5], left)

    def expert_hidden(g):
        while loads:
            loads.pop().wait()
        rows = a2d[g]
        by_unit = (((1,), (1,)), ((), ()))
        gate = lax.dot_general(rows, wg[...], by_unit, preferred_element_type=F32)
        up = lax.dot_general(rows, wu[...], by_unit, preferred_element_type=F32)
        hid[...] = (gate / (1.0 + jnp.exp(-gate)) * up).astype(BF16)

    def s3(g):
        arrive(a2d.at[g, rows_of(1), hi], ag_recv.at[g, 2])
        arrive(a2d.at[g, rows_of(2), lo], ag_recv.at[g, 3])
        arrive(a2d.at[g, rows_of(3), lo], ag_recv.at[g, 4])
        arrive(a2d.at[g, rows_of(3), hi], ag_recv.at[g, 5])
        expert_hidden(g)
        n_cols = half // 2
        for n in range(4):
            cols = slice(n * n_cols, (n + 1) * n_cols)
            res = jnp.dot(hid[...], wd[:, cols], preferred_element_type=F32)
            own[g, :, cols] = res[0:gr]
            to_left, to_right = res[gr : 2 * gr], res[2 * gr : 3 * gr]
            in_half = slice((n % 2) * n_cols, (n % 2 + 1) * n_cols)
            if n < 2:
                part[g, 0, :, cols] = to_left.astype(BF16)
                pf[g, 1, :, in_half] = to_right
            else:
                pf[g, 0, :, in_half] = to_left
                part[g, 1, :, cols] = to_right.astype(BF16)
            part[g, 2, :, cols] = res[3 * gr : 4 * gr].astype(BF16)
        push(part.at[g, 2, :, lo], rs1.at[g, 0], rs_send.at[g, 0], rs_recv.at[g, 0], right)
        push(part.at[g, 2, :, hi], rs1.at[g, 1], rs_send.at[g, 1], rs_recv.at[g, 1], left)
        push(part.at[g, 1, :, hi], rs2.at[g, 0, :, hi], rs_send.at[g, 2], rs_recv.at[g, 2], right)
        push(part.at[g, 0, :, lo], rs2.at[g, 1, :, lo], rs_send.at[g, 3], rs_recv.at[g, 3], left)

    def s4(g):
        arrive(rs1.at[g, 0], rs_recv.at[g, 0])
        part[g, 1, :, 0:half] = (pf[g, 1] + rs1[g, 0].astype(F32)).astype(BF16)
        push(part.at[g, 1, :, lo], rs2.at[g, 0, :, lo], rs_send.at[g, 4], rs_recv.at[g, 4], right)
        arrive(rs1.at[g, 1], rs_recv.at[g, 1])
        part[g, 0, :, half:width] = (pf[g, 0] + rs1[g, 1].astype(F32)).astype(BF16)
        push(part.at[g, 0, :, hi], rs2.at[g, 1, :, hi], rs_send.at[g, 5], rs_recv.at[g, 5], left)

    def s5(g):
        arrive(rs2.at[g, 0, :, hi], rs_recv.at[g, 2])
        arrive(rs2.at[g, 1, :, lo], rs_recv.at[g, 3])
        arrive(rs2.at[g, 0, :, lo], rs_recv.at[g, 4])
        arrive(rs2.at[g, 1, :, hi], rs_recv.at[g, 5])
        total = own[g] + rs2[g, 0].astype(F32) + rs2[g, 1].astype(F32)
        rows2d[...] = total.astype(BF16)
        to_tiles(rows2d, ret3, g * gr)
        exchange(ret3, back3, g, -1, back_send, back_recv)

    def s6(g):
        exchanged(back3, g, back_recv)
        from_tiles(block_in(back3, g * gr), rows2d)
        combine(g)

    def combine(g):
        rows = rows2d[...]
        res = jnp.dot(whi[g], rows, preferred_element_type=F32)
        res = res + jnp.dot(wlo[g], rows, preferred_element_type=F32)
        acc[...] = acc[...] + res

    top, low = pl.ds(0, gr // 2), pl.ds(gr // 2, gr - gr // 2)

    def n1():
        push(fx.at[0, top], fx.at[1, top], fx_send.at[0], fx_recv.at[0], right)
        push(fx.at[0, low], fx.at[2, low], fx_send.at[1], fx_recv.at[1], left)
        push(fx.at[0, low], fx.at[1, low], fx_send.at[2], fx_recv.at[2], right)
        push(fx.at[0, top], fx.at[2, top], fx_send.at[3], fx_recv.at[3], left)

    def n2():
        arrive(fx.at[1, top], fx_recv.at[0])
        push(fx.at[1, top], fx.at[3, top], fx_send.at[4], fx_recv.at[4], right)
        arrive(fx.at[2, low], fx_recv.at[1])
        push(fx.at[2, low], fx.at[3, low], fx_send.at[5], fx_recv.at[5], left)

    def n3():
        arrive(fx.at[1, low], fx_recv.at[2])
        arrive(fx.at[2, top], fx_recv.at[3])
        arrive(fx.at[3, top], fx_recv.at[4])
        arrive(fx.at[3, low], fx_recv.at[5])
        exchange(fx, fr, 0, 1, a2a_send, a2a_recv)

    def n4():
        exchanged(fr, 0, a2a_recv)
        for k in range(nx):
            from_tiles(block_in(fr.at[k], 0), a2d.at[0, rows_of(k)])
        expert_hidden(0)
        n_cols = width // 4
        for n in range(4):
            cols = slice(n * n_cols, (n + 1) * n_cols)
            a2d[0, :, cols] = jnp.dot(hid[...], wd[:, cols], preferred_element_type=F32).astype(BF16)
        for k in range(nx):
            to_tiles(a2d.at[0, rows_of(k)], fs.at[k], 0)
        exchange(fs, fb, 0, -1, back_send, back_recv)

    def n5():
        exchanged(fb, 0, back_recv)
        push(fb.at[3, top], f1.at[0], fb_send.at[0], fb_recv.at[0], right)
        push(fb.at[3, low], f1.at[1], fb_send.at[1], fb_recv.at[1], left)
        push(fb.at[2, low], f2.at[0, low], fb_send.at[2], fb_recv.at[2], right)
        push(fb.at[1, top], f2.at[1, top], fb_send.at[3], fb_recv.at[3], left)

    def n6():
        arrive(f1.at[0], fb_recv.at[0])
        fsum[0] = (fb[2, top].astype(F32) + f1[0].astype(F32)).astype(BF16)
        push(fsum.at[0], f2.at[0, top], fb_send.at[4], fb_recv.at[4], right)
        arrive(f1.at[1], fb_recv.at[1])
        fsum[1] = (fb[1, low].astype(F32) + f1[1].astype(F32)).astype(BF16)
        push(fsum.at[1], f2.at[1, low], fb_send.at[5], fb_recv.at[5], left)

    def n7():
        arrive(f2.at[0, low], fb_recv.at[2])
        arrive(f2.at[1, top], fb_recv.at[3])
        arrive(f2.at[0, top], fb_recv.at[4])
        arrive(f2.at[1, low], fb_recv.at[5])

        def summed(r):
            rows = slice(r, r + ROW_TILE)
            both = f2[0, rows].astype(F32) + f2[1, rows].astype(F32)
            return (fb[0, rows].astype(F32) + both).astype(BF16)

        from_tiles(summed, rows2d)
        combine(0)

    def send_counts():
        def one(i, carry):
            pltpu.make_async_remote_copy(
                src_ref=cnt_mine, dst_ref=cnt_all.at[i], send_sem=cnt_send, recv_sem=cnt_recv,
                device_id=relative(1, *split(i)), device_id_type=MESH,
            ).start()
            return carry

        lax.fori_loop(1, plane, one, 0)

    counted = {}

    def plane_counts():
        arrive(cnt_all.at[pl.ds(1, plane - 1)], cnt_recv)
        table = cnt_all[:, 0, 0:n_experts]
        i = lax.broadcasted_iota(I32, (plane, 1), 0)
        sz = (z - lax.shift_right_logical(i, log2(per_z)) + nz) & (nz - 1)
        sy = (y - (lax.shift_right_logical(i, log2(nc)) & (ny - 1)) + ny) & (ny - 1)
        sc = (c - (i & (nc - 1)) + nc) & (nc - 1)
        mine = (z * ny + y) * nc + c
        first = ((sz * ny + sy) * nc + sc < mine).astype(F32)
        counted["inside"] = jnp.sum(table * first, axis=0, keepdims=True)
        tot_mine[:, 0:n_experts] = jnp.sum(table, axis=0, keepdims=True)
        for k, new_x in enumerate((right, left, opp)):
            push(tot_mine, tot_all.at[k], tot_send.at[k], tot_recv.at[k], new_x)

    def weigh():
        small[2].wait()
        small[3].wait()
        offset = counted["inside"]
        for k, src in enumerate((left, right, opp)):
            arrive(tot_all.at[k], tot_recv.at[k])
            offset = offset + tot_all[k][:, 0:n_experts] * jnp.where(src < x, 1.0, 0.0)
        diagonal = lax.broadcasted_iota(I32, (n_experts, n_experts), 0) == lax.broadcasted_iota(
            I32, (n_experts, n_experts), 1
        )

        def down(row):
            return jnp.sum(jnp.where(diagonal, row, 0.0), axis=1, keepdims=True)

        offset, limit = down(offset), down(cap[...].astype(F32))
        parts = []
        for k, (oh, rank, pos) in enumerate(((oh0, rank0, pos0), (oh1, rank1, pos1))):
            slot = jnp.sum(oh * offset, axis=0, keepdims=True) + rank
            top = jnp.sum(oh * limit, axis=0, keepdims=True)
            unit = jnp.where(slot < top, units[k : k + 1, :], 0)
            high = unit & ~7
            parts.append((pos, high.astype(F32) / 1024.0, (unit - high).astype(F32) / 1024.0))
        wide = lax.broadcasted_iota(I32, (LANES, t_rows), 0)
        for g in range(len(groups)):
            h = l = jnp.zeros((LANES, t_rows), F32)
            for pos, high, low in parts:
                here = wide + g * gr == pos
                h, l = h + jnp.where(here, high, 0.0), l + jnp.where(here, low, 0.0)
            whi[g] = jnp.transpose(h)[:, 0:gr].astype(BF16)
            wlo[g] = jnp.transpose(l)[:, 0:gr].astype(BF16)
        acc[...] = jnp.zeros_like(acc)

    n = len(groups)
    steps = nz // 2 - 1

    def dispatch(g):
        gather(g)
        exchange(out3, recv3, g, 1, a2a_send, a2a_recv)

    def enter():
        gather(0)
        with jax.named_scope("barrier"):
            near_ready()

    def relay(step):
        told(step)
        if step + 1 < steps:
            tell(step + 1)

    if n == 4:
        order = [
            (enter,), (n1,), (tell, 0), (relay, 0), (dispatch, 3), (relay, 1), (n2,), (relay, 2), (dispatch, 1),
            (s1, 3), (dispatch, 2), (s2, 3), (s1, 1), (send_counts,), (onward, 0), (s2, 1), (n3,), (s1, 2), (s3, 1),
            (s2, 2), (n4,), (s4, 1), (s3, 2), (s5, 1), (plane_counts,), (s4, 2), (s3, 3), (s5, 2), (s4, 3), (n5,),
            (weigh,), (onward, 1), (s5, 3), (s6, 1), (n6,), (n7,), (s6, 2), (s6, 3),
        ]
    else:
        order = [(enter,), (n1,), (tell, 0)] + [(relay, step) for step in range(steps)]
        order += [(dispatch, g) for g in range(1, n)] + [(n2,), (n3,), (onward, 0)]
        order += [(stage, g) for stage in (s1, s2, s3, s4, s5) for g in range(1, n)]
        order += [(n4,), (send_counts,), (plane_counts,), (weigh,), (n5,), (n6,), (onward, 1)] + [(s6, g) for g in range(1, n)] + [(n7,)]
    for stage, *args in order:
        with jax.named_scope("_".join([stage.__name__, *map(str, args)])):
            stage(*args)
    out[...] = acc[...].astype(BF16)

    for copy in sent:
        copy.wait_send()
    exchanged(fx, 0, a2a_send)
    exchanged(fs, 0, back_send)
    for g in range(1, n):
        exchanged(out3, g, a2a_send)
        exchanged(ret3, g, back_send)
    arrive(cnt_all.at[pl.ds(1, plane - 1)], cnt_send)


def local(shape, most, tokens, expert_ids, gate_units, capacity, w_gate, w_up, w_down):
    nx, nz, ny, nc = shape
    t_rows, width = tokens.shape
    ff = w_gate.shape[2]
    turn = functools.partial(jnp.swapaxes, axis1=-1, axis2=-2)
    plane = nz * ny * nc
    groups = offset_groups(nz, ny)
    n, gr = len(groups), len(groups[0]) * nc * most
    vmem = pl.BlockSpec(memory_space=pltpu.VMEM)
    in_hbm = pl.BlockSpec(memory_space=pltpu.HBM)
    stay = functools.partial(pltpu.with_memory_space_constraint, memory_space=pltpu.HBM)
    dma = pltpu.SemaphoreType.DMA
    near_tiles = pltpu.VMEM((nx, gr, ROW_TILE, LANES), BF16)
    tiles = pltpu.VMEM((plane * most, ROW_TILE, LANES), BF16)
    return pl.pallas_call(
        functools.partial(kernel, shape, most),
        out_shape=jax.ShapeDtypeStruct((t_rows, width), BF16),
        in_specs=[in_hbm] * 7,
        out_specs=vmem,
        scratch_shapes=[
            pltpu.VMEM((t_rows, width), BF16),
            pltpu.VMEM((2, t_rows), I32),
            pltpu.VMEM((2, t_rows), I32),
            pltpu.VMEM((1, plane), I32),
            pltpu.VMEM((ff, width), BF16),
            pltpu.VMEM((ff, width), BF16),
            pltpu.VMEM((ff, width), BF16),
            pltpu.VMEM((256, 256), BF16),
            pltpu.VMEM((gr, width), BF16),
            tiles, tiles, tiles, tiles,
            pltpu.VMEM((n, nx * gr, width), BF16),
            pltpu.VMEM((nx * gr, ff), BF16),
            pltpu.VMEM((n, gr, width), F32),
            pltpu.VMEM((n, 2, gr, width // 2), F32),
            pltpu.VMEM((n, 3, gr, width), BF16),
            pltpu.VMEM((n, 2, gr, width // 2), BF16),
            pltpu.VMEM((n, 2, gr, width), BF16),
            pltpu.VMEM((8, LANES), F32),
            pltpu.VMEM((n, t_rows, gr), BF16),
            pltpu.VMEM((n, t_rows, gr), BF16),
            pltpu.VMEM((t_rows, width), F32),
            pltpu.VMEM((1, LANES), F32),
            pltpu.VMEM((plane, 1, LANES), F32),
            pltpu.VMEM((1, LANES), F32),
            pltpu.VMEM((3, 1, LANES), F32),
            near_tiles, near_tiles, near_tiles, near_tiles,
            pltpu.VMEM((2, gr // 2, ROW_TILE, LANES), BF16),
            pltpu.VMEM((2, gr, ROW_TILE, LANES), BF16),
            pltpu.VMEM((2, gr // 2, ROW_TILE, LANES), BF16),
            pltpu.VMEM((2, min(2, ny) * nc * most, ROW_TILE, LANES), BF16),
            pltpu.SemaphoreType.REGULAR((nz // 2 - 1,)),
            dma((7,)),
            dma((n,)), dma((n,)),
            dma((n, 6)), dma((n, 6)),
            dma((n, 6)), dma((n, 6)),
            dma((n,)), dma((n,)),
            dma, dma,
            dma((3,)), dma((3,)),
            dma((6,)), dma((6,)),
            dma((6,)), dma((6,)),
            dma((2,)), dma((2,)),
        ],
        compiler_params=pltpu.CompilerParams(collective_id=0, has_side_effects=True, vmem_limit_bytes=56000000),
    )(
        tokens, stay(turn(expert_ids)), stay(turn(gate_units)), stay(capacity.reshape(1, -1)),
        turn(w_gate), turn(w_up), turn(w_down),
    )


def build(finer, most):
    shape = tuple(finer.shape[a] for a in AXES)
    return jax.shard_map(
        functools.partial(local, shape, most),
        mesh=finer,
        in_specs=(
            P(AXES, None),
            P(AXES, None),
            P(AXES, None),
            P(),
            P(EXPERT, None, "dp"),
            P(EXPERT, None, "dp"),
            P(EXPERT, None, "dp"),
        ),
        out_specs=P(AXES, None),
        check_vma=False,
    )


def solution(mesh):
    finer = Mesh(mesh.devices.reshape(mesh.shape["dp"], 8, 4, 2), AXES)
    return build(finer, 5)
```

```python
import functools

import jax
import jax.numpy as jnp
from jax import lax
from jax.experimental import pallas as pl
from jax.experimental.pallas import tpu as pltpu
from jax.sharding import Mesh
from jax.sharding import PartitionSpec as P

MESH = pl.DeviceIdType.MESH
AXES = ("dp", "expert_0", "expert_1", "expert_2")
EXPERT = ("expert_0", "expert_1", "expert_2")
BF16, F32, I32 = jnp.bfloat16, jnp.float32, jnp.int32
LANES = 128
ROW_TILE = 16


def offset_groups(nz, ny):
    if (nz, ny) != (8, 4):
        first = [(dz, dy) for dz in (0, 1) for dy in range(ny)]
        return [first] + [
            [(dz, dy) for dz in (k + 1, -k) for dy in range(ny)] for k in reversed(range(1, nz // 2))
        ]
    return [
        [(0, 0), (0, 1), (0, 2), (0, 3), (1, 0), (-1, 0), (1, 3), (-1, 3)],
        [(-2, 2), (2, 2), (3, 0), (-3, 0), (3, 1), (-3, 1), (3, 2), (-3, 2)],
        [(4, 0), (4, 1), (-2, 3), (2, 3), (3, 3), (-3, 3), (4, 2), (4, 3)],
        [(1, 1), (-1, 1), (1, 2), (-1, 2), (2, 0), (-2, 0), (2, 1), (-2, 1)],
    ]


def log2(n):
    assert n & (n - 1) == 0
    return n.bit_length() - 1


def kernel(
    shape, most,
    tokens_h, ids_h, units_h, cap_h, wg_h, wu_h, wd_h, out,
    tokens, ids, units, cap, wg, wu, wd, perm, rows2d, out3, recv3, ret3, back3, a2d, hid, own, pf, part, rs1, rs2,
    sel, whi, wlo, acc, cnt_mine, cnt_all, tot_mine, tot_all,
    fx, fr, fs, fb, f1, f2, fsum, relayed,
    near, w_sem, a2a_send, a2a_recv, ag_send, ag_recv, rs_send, rs_recv, back_send, back_recv, cnt_send, cnt_recv, tot_send, tot_recv,
    fx_send, fx_recv, fb_send, fb_recv, relay_send, relay_recv,
):
    nx, nz, ny, nc = shape
    x, z, y, c = (lax.axis_index(a) for a in AXES)
    right, left, opp = lax.rem(x + 1, nx), lax.rem(x + nx - 1, nx), lax.rem(x + 2, nx)
    plane = nz * ny * nc
    per_z = ny * nc
    groups = offset_groups(nz, ny)
    per_group = len(groups[0]) * nc
    far = [g for g, group in enumerate(groups) if group[0][0] == nz // 2 > 1]
    far_offsets = min(2, ny)
    gr = per_group * most
    blocks = gr // ROW_TILE
    t_rows, width = tokens.shape
    half = width // 2
    lo, hi = pl.ds(0, half), pl.ds(half, half)

    def at_x(new_x):
        return (new_x, z, y, c)

    def relative(sign, dz, dy, dc):
        return (
            x,
            lax.rem(z + sign * dz + 2 * nz, nz),
            lax.rem(y + sign * dy + ny, ny),
            lax.rem(c + sign * dc + nc, nc),
        )

    def split(i):
        return i // per_z, lax.rem(i // nc, ny), lax.rem(i, nc)

    barrier = pltpu.get_barrier_semaphore()
    nearby = min(3, nz) * per_z

    def greet(i, carry):
        dz, dy, dc = split(i)
        dz = jnp.where(dz == 2, -1, dz)
        pl.semaphore_signal(barrier, inc=1, device_id=relative(1, dz, dy, dc), device_id_type=MESH)
        return carry

    for new_x in (right, left, opp):
        pl.semaphore_signal(barrier, inc=1, device_id=at_x(new_x), device_id_type=MESH)
    lax.fori_loop(1, nearby, greet, 0)

    small = [
        pltpu.make_async_copy(src, dst, w_sem.at[i])
        for i, (src, dst) in enumerate(((ids_h, ids), (tokens_h, tokens), (units_h, units), (cap_h, cap)))
    ]
    loads = [
        pltpu.make_async_copy(src.at[0], dst, w_sem.at[4 + i])
        for i, (src, dst) in enumerate(((wg_h, wg), (wu_h, wu), (wd_h, wd)))
    ]
    for load in small + loads:
        load.start()

    def near_ready():
        pl.semaphore_wait(barrier, nearby - 1 + nx - 1)

    def tell(step):
        for dz in (1, -1):
            pl.semaphore_signal(near.at[step], inc=1, device_id=relative(1, dz, 0, 0), device_id_type=MESH)

    def told(step):
        pl.semaphore_wait(near.at[step], 2)

    i_row = lax.broadcasted_iota(I32, (256, 256), 0)
    i_col = lax.broadcasted_iota(I32, (256, 256), 1)
    swapped = (i_row & 15) * 16 + lax.shift_right_logical(i_row, 4)
    perm[...] = (i_col == swapped).astype(BF16)
    small[0].wait()

    n_experts = cap.shape[1]
    expert = lax.broadcasted_iota(I32, (n_experts, t_rows), 0)
    id0, id1 = ids[0:1, :], ids[1:2, :]
    oh0, oh1 = (expert == id0).astype(F32), (expert == id1).astype(F32)
    named = (oh0 + oh1).astype(BF16)
    counts = lax.dot_general(
        jnp.ones((8, t_rows), BF16), named, (((1,), (1,)), ((), ())), preferred_element_type=F32
    )[0:1, :]
    cnt_mine[:, 0:n_experts] = counts
    cnt_all[0, :, 0:n_experts] = counts
    earlier = (
        lax.broadcasted_iota(I32, (t_rows, t_rows), 0) < lax.broadcasted_iota(I32, (t_rows, t_rows), 1)
    ).astype(BF16)
    before = jnp.dot(named, earlier, preferred_element_type=F32)
    rank0 = jnp.sum(before * oh0, axis=0, keepdims=True)
    rank1 = jnp.sum(before * oh1, axis=0, keepdims=True)

    def slot_of(expert, rank):
        ez = lax.shift_right_logical(expert, log2(per_z))
        ey = lax.shift_right_logical(expert, log2(nc)) & (ny - 1)
        ec = expert & (nc - 1)
        dz = (ez - z + nz) & (nz - 1)
        dy = (ey - y + ny) & (ny - 1)
        dc = (ec - c + nc) & (nc - 1)
        key, place = dz * ny + dy, jnp.zeros_like(dz)
        for i, (z_off, y_off) in enumerate(pair for group in groups for pair in group):
            place = jnp.where(key == (z_off % nz) * ny + y_off, i, place)
        return (place * nc + dc) * most + rank.astype(I32)

    pos0, pos1 = slot_of(id0, rank0), slot_of(id1, rank1)
    small[1].wait()

    def to_tiles(src, dst3, r0):
        for b in range(blocks):
            block = src[ROW_TILE * b : ROW_TILE * (b + 1), :]
            stacked = jnp.concatenate(
                [block[:, LANES * s : LANES * (s + 1)] for s in range(width // LANES)], axis=0
            )
            turned = jnp.dot(perm[...], stacked, preferred_element_type=F32).astype(BF16)
            r = r0 + ROW_TILE * b
            dst3[r : r + ROW_TILE] = turned.reshape(ROW_TILE, ROW_TILE, LANES)

    def from_tiles(block_of, dst):
        for b in range(blocks):
            stacked = block_of(ROW_TILE * b).reshape(ROW_TILE * ROW_TILE, LANES)
            turned = jnp.dot(perm[...], stacked, preferred_element_type=F32).astype(BF16)
            for s in range(width // LANES):
                dst[ROW_TILE * b : ROW_TILE * (b + 1), LANES * s : LANES * (s + 1)] = turned[
                    ROW_TILE * s : ROW_TILE * (s + 1), :
                ]

    def block_in(src3, r0):
        return lambda r: src3[r0 + r : r0 + r + ROW_TILE]

    def exchange(src, dst, g, sign, send_sem, recv_sem):
        base = g * per_group if g else 0
        for i, (dz, dy) in enumerate(groups[g]):
            for dc in range(nc):
                rows = pl.ds((base + i * nc + dc) * most, most)
                rows = rows if g else (slice(None), rows)
                if dz == dy == dc == 0:
                    assert i == 0
                    continue
                target, arrival, z_off = dst.at[rows], recv_sem.at[g], sign * dz
                if g in far and i < far_offsets:
                    way = 0 if sign == 1 else 1
                    target = relayed.at[way, pl.ds((i * nc + dc) * most, most)]
                    arrival, z_off = relay_recv.at[way], -(nz // 4)
                pltpu.make_async_remote_copy(
                    src_ref=src.at[rows],
                    dst_ref=target,
                    send_sem=send_sem.at[g],
                    recv_sem=arrival,
                    device_id=relative(1, z_off, sign * dy, sign * dc),
                    device_id_type=MESH,
                ).start()
        if g == 0:
            dst[:, 0:most] = src[:, 0:most]

    def exchanged(ref, g, sem):
        rows = pl.ds(g * per_group * most, per_group * most)
        if g == 0:
            rows = (slice(None), pl.ds(most, (per_group - 1) * most))
        with jax.named_scope("wait"):
            pltpu.make_async_copy(ref.at[rows], ref.at[rows], sem.at[g]).wait()

    slots = lax.broadcasted_iota(I32, (gr, t_rows), 0)

    def gather(g):
        s0, s1 = (slots + g * gr == pos0), (slots + g * gr == pos1)
        chosen = (s0.astype(F32) + s1.astype(F32)).astype(BF16)
        rows = jnp.dot(chosen, tokens[...], preferred_element_type=F32)
        rows2d[...] = rows.astype(BF16)
        if g:
            to_tiles(rows2d, out3, g * gr)
        else:
            to_tiles(rows2d, fx.at[0], 0)

    sent = []

    def push(src, dst, send_sem, recv_sem, new_x):
        copy = pltpu.make_async_remote_copy(
            src_ref=src, dst_ref=dst, send_sem=send_sem, recv_sem=recv_sem,
            device_id=at_x(new_x), device_id_type=MESH,
        )
        copy.start()
        sent.append(copy)

    def arrive(ref, sem):
        with jax.named_scope("wait"):
            pltpu.make_async_copy(ref, ref, sem).wait()

    def rows_of(slot):
        return pl.ds(slot * gr, gr)

    def onward(way):
        (g,) = far
        rows = pl.ds(g * per_group * most, far_offsets * nc * most)
        dst, recv_sem = ((recv3, a2a_recv), (back3, back_recv))[way]
        arrive(relayed.at[way], relay_recv.at[way])
        copy = pltpu.make_async_remote_copy(
            src_ref=relayed.at[way], dst_ref=dst.at[rows], send_sem=relay_send.at[way], recv_sem=recv_sem.at[g],
            device_id=relative(1, -(nz // 4), 0, 0), device_id_type=MESH,
        )
        copy.start()
        sent.append(copy)

    def s1(g):
        exchanged(recv3, g, a2a_recv)
        from_tiles(block_in(recv3, g * gr), a2d.at[g])
        me = rows_of(0)
        push(a2d.at[g, me, lo], a2d.at[g, rows_of(1), lo], ag_send.at[g, 0], ag_recv.at[g, 0], right)
        push(a2d.at[g, me, hi], a2d.at[g, rows_of(2), hi], ag_send.at[g, 1], ag_recv.at[g, 1], left)
        push(a2d.at[g, me, hi], a2d.at[g, rows_of(1), hi], ag_send.at[g, 2], ag_recv.at[g, 2], right)
        push(a2d.at[g, me, lo], a2d.at[g, rows_of(2), lo], ag_send.at[g, 3], ag_recv.at[g, 3], left)

    def s2(g):
        arrive(a2d.at[g, rows_of(1), lo], ag_recv.at[g, 0])
        push(a2d.at[g, rows_of(1), lo], a2d.at[g, rows_of(3), lo], ag_send.at[g, 4], ag_recv.at[g, 4], right)
        arrive(a2d.at[g, rows_of(2), hi], ag_recv.at[g, 1])
        push(a2d.at[g, rows_of(2), hi], a2d.at[g, rows_of(3), hi], ag_send.at[g, 5], ag_recv.at[g, 5], left)

    def expert_hidden(g):
        while loads:
            loads.pop().wait()
        rows = a2d[g]
        by_unit = (((1,), (1,)), ((), ()))
        gate = lax.dot_general(rows, wg[...], by_unit, preferred_element_type=F32)
        up = lax.dot_general(rows, wu[...], by_unit, preferred_element_type=F32)
        hid[...] = (gate / (1.0 + jnp.exp(-gate)) * up).astype(BF16)

    def s3(g):
        arrive(a2d.at[g, rows_of(1), hi], ag_recv.at[g, 2])
        arrive(a2d.at[g, rows_of(2), lo], ag_recv.at[g, 3])
        arrive(a2d.at[g, rows_of(3), lo], ag_recv.at[g, 4])
        arrive(a2d.at[g, rows_of(3), hi], ag_recv.at[g, 5])
        expert_hidden(g)
        n_cols = half // 2
        for n in range(4):
            cols = slice(n * n_cols, (n + 1) * n_cols)
            res = jnp.dot(hid[...], wd[:, cols], preferred_element_type=F32)
            own[g, :, cols] = res[0:gr]
            to_left, to_right = res[gr : 2 * gr], res[2 * gr : 3 * gr]
            in_half = slice((n % 2) * n_cols, (n % 2 + 1) * n_cols)
            if n < 2:
                part[g, 0, :, cols] = to_left.astype(BF16)
                pf[g, 1, :, in_half] = to_right
            else:
                pf[g, 0, :, in_half] = to_left
                part[g, 1, :, cols] = to_right.astype(BF16)
            part[g, 2, :, cols] = res[3 * gr : 4 * gr].astype(BF16)
        push(part.at[g, 2, :, lo], rs1.at[g, 0], rs_send.at[g, 0], rs_recv.at[g, 0], right)
        push(part.at[g, 2, :, hi], rs1.at[g, 1], rs_send.at[g, 1], rs_recv.at[g, 1], left)
        push(part.at[g, 1, :, hi], rs2.at[g, 0, :, hi], rs_send.at[g, 2], rs_recv.at[g, 2], right)
        push(part.at[g, 0, :, lo], rs2.at[g, 1, :, lo], rs_send.at[g, 3], rs_recv.at[g, 3], left)

    def s4(g):
        arrive(rs1.at[g, 0], rs_recv.at[g, 0])
        part[g, 1, :, 0:half] = (pf[g, 1] + rs1[g, 0].astype(F32)).astype(BF16)
        push(part.at[g, 1, :, lo], rs2.at[g, 0, :, lo], rs_send.at[g, 4], rs_recv.at[g, 4], right)
        arrive(rs1.at[g, 1], rs_recv.at[g, 1])
        part[g, 0, :, half:width] = (pf[g, 0] + rs1[g, 1].astype(F32)).astype(BF16)
        push(part.at[g, 0, :, hi], rs2.at[g, 1, :, hi], rs_send.at[g, 5], rs_recv.at[g, 5], left)

    def s5(g):
        arrive(rs2.at[g, 0, :, hi], rs_recv.at[g, 2])
        arrive(rs2.at[g, 1, :, lo], rs_recv.at[g, 3])
        arrive(rs2.at[g, 0, :, lo], rs_recv.at[g, 4])
        arrive(rs2.at[g, 1, :, hi], rs_recv.at[g, 5])
        total = own[g] + rs2[g, 0].astype(F32) + rs2[g, 1].astype(F32)
        rows2d[...] = total.astype(BF16)
        to_tiles(rows2d, ret3, g * gr)
        exchange(ret3, back3, g, -1, back_send, back_recv)

    def s6(g):
        exchanged(back3, g, back_recv)
        from_tiles(block_in(back3, g * gr), rows2d)
        combine(g)

    combined = []

    def combine(g):
        rows = rows2d[...]
        res = jnp.dot(whi[g], rows, preferred_element_type=F32)
        res = res + jnp.dot(wlo[g], rows, preferred_element_type=F32)
        combined.append(g)
        if len(combined) == len(groups):
            out[...] = (acc[...] + res).astype(BF16)
        elif len(combined) == 1:
            acc[...] = res
        else:
            acc[...] = acc[...] + res

    top, low = pl.ds(0, gr // 2), pl.ds(gr // 2, gr - gr // 2)

    def n1():
        push(fx.at[0, top], fx.at[1, top], fx_send.at[0], fx_recv.at[0], right)
        push(fx.at[0, low], fx.at[2, low], fx_send.at[1], fx_recv.at[1], left)
        push(fx.at[0, low], fx.at[1, low], fx_send.at[2], fx_recv.at[2], right)
        push(fx.at[0, top], fx.at[2, top], fx_send.at[3], fx_recv.at[3], left)

    def n2():
        arrive(fx.at[1, top], fx_recv.at[0])
        push(fx.at[1, top], fx.at[3, top], fx_send.at[4], fx_recv.at[4], right)
        arrive(fx.at[2, low], fx_recv.at[1])
        push(fx.at[2, low], fx.at[3, low], fx_send.at[5], fx_recv.at[5], left)

    def n3():
        arrive(fx.at[1, low], fx_recv.at[2])
        arrive(fx.at[2, top], fx_recv.at[3])
        arrive(fx.at[3, top], fx_recv.at[4])
        arrive(fx.at[3, low], fx_recv.at[5])
        exchange(fx, fr, 0, 1, a2a_send, a2a_recv)

    def n4():
        exchanged(fr, 0, a2a_recv)
        for k in range(nx):
            from_tiles(block_in(fr.at[k], 0), a2d.at[0, rows_of(k)])
        expert_hidden(0)
        n_cols = width // 4
        for n in range(4):
            cols = slice(n * n_cols, (n + 1) * n_cols)
            a2d[0, :, cols] = jnp.dot(hid[...], wd[:, cols], preferred_element_type=F32).astype(BF16)
        for k in range(nx):
            to_tiles(a2d.at[0, rows_of(k)], fs.at[k], 0)
        exchange(fs, fb, 0, -1, back_send, back_recv)

    def n5():
        exchanged(fb, 0, back_recv)
        push(fb.at[3, top], f1.at[0], fb_send.at[0], fb_recv.at[0], right)
        push(fb.at[3, low], f1.at[1], fb_send.at[1], fb_recv.at[1], left)
        push(fb.at[2, low], f2.at[0, low], fb_send.at[2], fb_recv.at[2], right)
        push(fb.at[1, top], f2.at[1, top], fb_send.at[3], fb_recv.at[3], left)

    def n6():
        arrive(f1.at[0], fb_recv.at[0])
        fsum[0] = (fb[2, top].astype(F32) + f1[0].astype(F32)).astype(BF16)
        push(fsum.at[0], f2.at[0, top], fb_send.at[4], fb_recv.at[4], right)
        arrive(f1.at[1], fb_recv.at[1])
        fsum[1] = (fb[1, low].astype(F32) + f1[1].astype(F32)).astype(BF16)
        push(fsum.at[1], f2.at[1, low], fb_send.at[5], fb_recv.at[5], left)

    def n7():
        arrive(f2.at[0, low], fb_recv.at[2])
        arrive(f2.at[1, top], fb_recv.at[3])
        arrive(f2.at[0, top], fb_recv.at[4])
        arrive(f2.at[1, low], fb_recv.at[5])

        def summed(r):
            rows = slice(r, r + ROW_TILE)
            both = f2[0, rows].astype(F32) + f2[1, rows].astype(F32)
            return (fb[0, rows].astype(F32) + both).astype(BF16)

        from_tiles(summed, rows2d)
        combine(0)

    def send_counts():
        def one(i, carry):
            pltpu.make_async_remote_copy(
                src_ref=cnt_mine, dst_ref=cnt_all.at[i], send_sem=cnt_send, recv_sem=cnt_recv,
                device_id=relative(1, *split(i)), device_id_type=MESH,
            ).start()
            return carry

        lax.fori_loop(1, plane, one, 0)

    counted = {}

    def plane_counts():
        arrive(cnt_all.at[pl.ds(1, plane - 1)], cnt_recv)
        table = cnt_all[:, 0, 0:n_experts]
        i = lax.broadcasted_iota(I32, (plane, 1), 0)
        sz = (z - lax.shift_right_logical(i, log2(per_z)) + nz) & (nz - 1)
        sy = (y - (lax.shift_right_logical(i, log2(nc)) & (ny - 1)) + ny) & (ny - 1)
        sc = (c - (i & (nc - 1)) + nc) & (nc - 1)
        mine = (z * ny + y) * nc + c
        first = ((sz * ny + sy) * nc + sc < mine).astype(F32)
        counted["inside"] = jnp.sum(table * first, axis=0, keepdims=True)
        tot_mine[:, 0:n_experts] = jnp.sum(table, axis=0, keepdims=True)
        for k, new_x in enumerate((right, left, opp)):
            push(tot_mine, tot_all.at[k], tot_send.at[k], tot_recv.at[k], new_x)

    def weigh():
        small[2].wait()
        small[3].wait()
        offset = counted["inside"]
        for k, src in enumerate((left, right, opp)):
            arrive(tot_all.at[k], tot_recv.at[k])
            offset = offset + tot_all[k][:, 0:n_experts] * jnp.where(src < x, 1.0, 0.0)
        diagonal = lax.broadcasted_iota(I32, (n_experts, n_experts), 0) == lax.broadcasted_iota(
            I32, (n_experts, n_experts), 1
        )

        def down(row):
            return jnp.sum(jnp.where(diagonal, row, 0.0), axis=1, keepdims=True)

        offset, limit = down(offset), down(cap[...].astype(F32))
        parts = []
        for k, (oh, rank, pos) in enumerate(((oh0, rank0, pos0), (oh1, rank1, pos1))):
            slot = jnp.sum(oh * offset, axis=0, keepdims=True) + rank
            top = jnp.sum(oh * limit, axis=0, keepdims=True)
            unit = jnp.where(slot < top, units[k : k + 1, :], 0)
            high = unit & ~7
            parts.append((pos, high.astype(F32) / 1024.0, (unit - high).astype(F32) / 1024.0))
        wide = lax.broadcasted_iota(I32, (LANES, t_rows), 0)
        for g in range(len(groups)):
            h = l = jnp.zeros((LANES, t_rows), F32)
            for pos, high, low in parts:
                here = wide + g * gr == pos
                h, l = h + jnp.where(here, high, 0.0), l + jnp.where(here, low, 0.0)
            whi[g] = jnp.transpose(h)[:, 0:gr].astype(BF16)
            wlo[g] = jnp.transpose(l)[:, 0:gr].astype(BF16)

    n = len(groups)
    steps = nz // 2 - 1

    def dispatch(g):
        gather(g)
        exchange(out3, recv3, g, 1, a2a_send, a2a_recv)

    def enter():
        gather(0)
        with jax.named_scope("barrier"):
            near_ready()

    def relay(step):
        told(step)
        if step + 1 < steps:
            tell(step + 1)

    if n == 4:
        order = [
            (enter,), (n1,), (tell, 0), (relay, 0), (dispatch, 3), (relay, 1), (n2,), (relay, 2), (dispatch, 1),
            (s1, 3), (dispatch, 2), (s2, 3), (s1, 1), (send_counts,), (onward, 0), (s2, 1), (n3,), (s1, 2), (s3, 1),
            (s2, 2), (n4,), (s4, 1), (s3, 2), (s5, 1), (plane_counts,), (s4, 2), (s3, 3), (s5, 2), (s4, 3), (n5,),
            (weigh,), (onward, 1), (s5, 3), (s6, 1), (n6,), (n7,), (s6, 2), (s6, 3),
        ]
    else:
        order = [(enter,), (n1,), (tell, 0)] + [(relay, step) for step in range(steps)]
        order += [(dispatch, g) for g in range(1, n)] + [(n2,), (n3,), (onward, 0)]
        order += [(stage, g) for stage in (s1, s2, s3, s4, s5) for g in range(1, n)]
        order += [(n4,), (send_counts,), (plane_counts,), (weigh,), (n5,), (n6,), (onward, 1)] + [(s6, g) for g in range(1, n)] + [(n7,)]
    for stage, *args in order:
        with jax.named_scope("_".join([stage.__name__, *map(str, args)])):
            stage(*args)

    for copy in sent:
        copy.wait_send()
    exchanged(fx, 0, a2a_send)
    exchanged(fs, 0, back_send)
    for g in range(1, n):
        exchanged(out3, g, a2a_send)
        exchanged(ret3, g, back_send)
    arrive(cnt_all.at[pl.ds(1, plane - 1)], cnt_send)


def local(shape, most, tokens, expert_ids, gate_units, capacity, w_gate, w_up, w_down):
    nx, nz, ny, nc = shape
    t_rows, width = tokens.shape
    ff = w_gate.shape[2]
    turn = functools.partial(jnp.swapaxes, axis1=-1, axis2=-2)
    plane = nz * ny * nc
    groups = offset_groups(nz, ny)
    n, gr = len(groups), len(groups[0]) * nc * most
    vmem = pl.BlockSpec(memory_space=pltpu.VMEM)
    in_hbm = pl.BlockSpec(memory_space=pltpu.HBM)
    stay = functools.partial(pltpu.with_memory_space_constraint, memory_space=pltpu.HBM)
    dma = pltpu.SemaphoreType.DMA
    near_tiles = pltpu.VMEM((nx, gr, ROW_TILE, LANES), BF16)
    tiles = pltpu.VMEM((plane * most, ROW_TILE, LANES), BF16)
    return pl.pallas_call(
        functools.partial(kernel, shape, most),
        out_shape=jax.ShapeDtypeStruct((t_rows, width), BF16),
        in_specs=[in_hbm] * 7,
        out_specs=vmem,
        scratch_shapes=[
            pltpu.VMEM((t_rows, width), BF16),
            pltpu.VMEM((2, t_rows), I32),
            pltpu.VMEM((2, t_rows), I32),
            pltpu.VMEM((1, plane), I32),
            pltpu.VMEM((ff, width), BF16),
            pltpu.VMEM((ff, width), BF16),
            pltpu.VMEM((ff, width), BF16),
            pltpu.VMEM((256, 256), BF16),
            pltpu.VMEM((gr, width), BF16),
            tiles, tiles, tiles, tiles,
            pltpu.VMEM((n, nx * gr, width), BF16),
            pltpu.VMEM((nx * gr, ff), BF16),
            pltpu.VMEM((n, gr, width), F32),
            pltpu.VMEM((n, 2, gr, width // 2), F32),
            pltpu.VMEM((n, 3, gr, width), BF16),
            pltpu.VMEM((n, 2, gr, width // 2), BF16),
            pltpu.VMEM((n, 2, gr, width), BF16),
            pltpu.VMEM((8, LANES), F32),
            pltpu.VMEM((n, t_rows, gr), BF16),
            pltpu.VMEM((n, t_rows, gr), BF16),
            pltpu.VMEM((t_rows, width), F32),
            pltpu.VMEM((1, LANES), F32),
            pltpu.VMEM((plane, 1, LANES), F32),
            pltpu.VMEM((1, LANES), F32),
            pltpu.VMEM((3, 1, LANES), F32),
            near_tiles, near_tiles, near_tiles, near_tiles,
            pltpu.VMEM((2, gr // 2, ROW_TILE, LANES), BF16),
            pltpu.VMEM((2, gr, ROW_TILE, LANES), BF16),
            pltpu.VMEM((2, gr // 2, ROW_TILE, LANES), BF16),
            pltpu.VMEM((2, min(2, ny) * nc * most, ROW_TILE, LANES), BF16),
            pltpu.SemaphoreType.REGULAR((nz // 2 - 1,)),
            dma((7,)),
            dma((n,)), dma((n,)),
            dma((n, 6)), dma((n, 6)),
            dma((n, 6)), dma((n, 6)),
            dma((n,)), dma((n,)),
            dma, dma,
            dma((3,)), dma((3,)),
            dma((6,)), dma((6,)),
            dma((6,)), dma((6,)),
            dma((2,)), dma((2,)),
        ],
        compiler_params=pltpu.CompilerParams(collective_id=0, has_side_effects=True, vmem_limit_bytes=56000000),
    )(
        tokens, stay(turn(expert_ids)), stay(turn(gate_units)), stay(capacity.reshape(1, -1)),
        turn(w_gate), turn(w_up), turn(w_down),
    )


def build(finer, most):
    shape = tuple(finer.shape[a] for a in AXES)
    return jax.shard_map(
        functools.partial(local, shape, most),
        mesh=finer,
        in_specs=(
            P(AXES, None),
            P(AXES, None),
            P(AXES, None),
            P(),
            P(EXPERT, None, "dp"),
            P(EXPERT, None, "dp"),
            P(EXPERT, None, "dp"),
        ),
        out_specs=P(AXES, None),
        check_vma=False,
    )


def solution(mesh):
    finer = Mesh(mesh.devices.reshape(mesh.shape["dp"], 8, 4, 2), AXES)
    return build(finer, 5)
```

```python
import functools

import jax
import jax.numpy as jnp
from jax import lax
from jax.experimental import pallas as pl
from jax.experimental.pallas import tpu as pltpu
from jax.sharding import Mesh
from jax.sharding import PartitionSpec as P

MESH = pl.DeviceIdType.MESH
AXES = ("dp", "expert_0", "expert_1", "expert_2")
EXPERT = ("expert_0", "expert_1", "expert_2")
BF16, F32, I32 = jnp.bfloat16, jnp.float32, jnp.int32
LANES = 128
ROW_TILE = 16


def offset_groups(nz, ny):
    if (nz, ny) != (8, 4):
        first = [(dz, dy) for dz in (0, 1) for dy in range(ny)]
        return [first] + [
            [(dz, dy) for dz in (k + 1, -k) for dy in range(ny)] for k in reversed(range(1, nz // 2))
        ]
    return [
        [(0, 0), (0, 1), (0, 2), (0, 3), (1, 0), (-1, 0), (1, 3), (-1, 3)],
        [(-2, 2), (2, 2), (3, 0), (-3, 0), (3, 1), (-3, 1), (3, 2), (-3, 2)],
        [(4, 0), (4, 1), (-2, 3), (2, 3), (3, 3), (-3, 3), (4, 2), (4, 3)],
        [(1, 1), (-1, 1), (1, 2), (-1, 2), (2, 0), (-2, 0), (2, 1), (-2, 1)],
    ]


def log2(n):
    assert n & (n - 1) == 0
    return n.bit_length() - 1


def kernel(
    shape, most,
    tokens_h, ids_h, units_h, cap_h, wg_h, wu_h, wd_h, out,
    tokens, ids, units, cap, wg, wu, wd, perm, rows2d, out3, recv3, ret3, back3, a2d, hid, own, pf, part, rs1, rs2,
    sel, whi, wlo, acc, cnt_mine, cnt_all, tot_mine, tot_all,
    fx, fr, fs, fb, f1, f2, fsum, relayed,
    near, w_sem, a2a_send, a2a_recv, ag_send, ag_recv, rs_send, rs_recv, back_send, back_recv, cnt_send, cnt_recv, tot_send, tot_recv,
    fx_send, fx_recv, fb_send, fb_recv, relay_send, relay_recv,
):
    nx, nz, ny, nc = shape
    x, z, y, c = (lax.axis_index(a) for a in AXES)
    right, left, opp = lax.rem(x + 1, nx), lax.rem(x + nx - 1, nx), lax.rem(x + 2, nx)
    plane = nz * ny * nc
    per_z = ny * nc
    groups = offset_groups(nz, ny)
    per_group = len(groups[0]) * nc
    far = [g for g, group in enumerate(groups) if group[0][0] == nz // 2 > 1]
    far_offsets = min(2, ny)
    gr = per_group * most
    blocks = gr // ROW_TILE
    t_rows, width = tokens.shape
    half = width // 2
    lo, hi = pl.ds(0, half), pl.ds(half, half)

    def at_x(new_x):
        return (new_x, z, y, c)

    def relative(sign, dz, dy, dc):
        return (
            x,
            lax.rem(z + sign * dz + 2 * nz, nz),
            lax.rem(y + sign * dy + ny, ny),
            lax.rem(c + sign * dc + nc, nc),
        )

    def split(i):
        return i // per_z, lax.rem(i // nc, ny), lax.rem(i, nc)

    barrier = pltpu.get_barrier_semaphore()
    nearby = min(3, nz) * per_z

    def greet(i, carry):
        dz, dy, dc = split(i)
        dz = jnp.where(dz == 2, -1, dz)
        pl.semaphore_signal(barrier, inc=1, device_id=relative(1, dz, dy, dc), device_id_type=MESH)
        return carry

    for new_x in (right, left, opp):
        pl.semaphore_signal(barrier, inc=1, device_id=at_x(new_x), device_id_type=MESH)
    lax.fori_loop(1, nearby, greet, 0)

    small = [
        pltpu.make_async_copy(src, dst, w_sem.at[i])
        for i, (src, dst) in enumerate(((ids_h, ids), (tokens_h, tokens), (units_h, units), (cap_h, cap)))
    ]
    loads = [
        pltpu.make_async_copy(src.at[0], dst, w_sem.at[4 + i])
        for i, (src, dst) in enumerate(((wg_h, wg), (wu_h, wu), (wd_h, wd)))
    ]
    for load in small + loads:
        load.start()

    def near_ready():
        pl.semaphore_wait(barrier, nearby - 1 + nx - 1)

    def tell(step):
        for dz in (1, -1):
            pl.semaphore_signal(near.at[step], inc=1, device_id=relative(1, dz, 0, 0), device_id_type=MESH)

    def told(step):
        pl.semaphore_wait(near.at[step], 2)

    i_row = lax.broadcasted_iota(I32, (256, 256), 0)
    i_col = lax.broadcasted_iota(I32, (256, 256), 1)
    swapped = (i_row & 15) * 16 + lax.shift_right_logical(i_row, 4)
    perm[...] = (i_col == swapped).astype(BF16)
    small[0].wait()

    n_experts = cap.shape[1]
    expert = lax.broadcasted_iota(I32, (n_experts, t_rows), 0)
    id0, id1 = ids[0:1, :], ids[1:2, :]
    oh0, oh1 = (expert == id0).astype(F32), (expert == id1).astype(F32)
    named = (oh0 + oh1).astype(BF16)
    counts = lax.dot_general(
        jnp.ones((8, t_rows), BF16), named, (((1,), (1,)), ((), ())), preferred_element_type=F32
    )[0:1, :]
    cnt_mine[:, 0:n_experts] = counts
    cnt_all[0, :, 0:n_experts] = counts
    earlier = (
        lax.broadcasted_iota(I32, (t_rows, t_rows), 0) < lax.broadcasted_iota(I32, (t_rows, t_rows), 1)
    ).astype(BF16)
    before = jnp.dot(named, earlier, preferred_element_type=F32)
    rank0 = jnp.sum(before * oh0, axis=0, keepdims=True)
    rank1 = jnp.sum(before * oh1, axis=0, keepdims=True)

    def slot_of(expert, rank):
        ez = lax.shift_right_logical(expert, log2(per_z))
        ey = lax.shift_right_logical(expert, log2(nc)) & (ny - 1)
        ec = expert & (nc - 1)
        dz = (ez - z + nz) & (nz - 1)
        dy = (ey - y + ny) & (ny - 1)
        dc = (ec - c + nc) & (nc - 1)
        key, place = dz * ny + dy, jnp.zeros_like(dz)
        for i, (z_off, y_off) in enumerate(pair for group in groups for pair in group):
            place = jnp.where(key == (z_off % nz) * ny + y_off, i, place)
        return (place * nc + dc) * most + rank.astype(I32)

    pos0, pos1 = slot_of(id0, rank0), slot_of(id1, rank1)
    small[1].wait()

    def to_tiles(src, dst3, r0):
        for b in range(blocks):
            block = src[ROW_TILE * b : ROW_TILE * (b + 1), :]
            stacked = jnp.concatenate(
                [block[:, LANES * s : LANES * (s + 1)] for s in range(width // LANES)], axis=0
            )
            turned = jnp.dot(perm[...], stacked, preferred_element_type=F32).astype(BF16)
            r = r0 + ROW_TILE * b
            dst3[r : r + ROW_TILE] = turned.reshape(ROW_TILE, ROW_TILE, LANES)

    def from_tiles(block_of, dst):
        for b in range(blocks):
            stacked = block_of(ROW_TILE * b).reshape(ROW_TILE * ROW_TILE, LANES)
            turned = jnp.dot(perm[...], stacked, preferred_element_type=F32).astype(BF16)
            for s in range(width // LANES):
                dst[ROW_TILE * b : ROW_TILE * (b + 1), LANES * s : LANES * (s + 1)] = turned[
                    ROW_TILE * s : ROW_TILE * (s + 1), :
                ]

    def block_in(src3, r0):
        return lambda r: src3[r0 + r : r0 + r + ROW_TILE]

    def exchange(src, dst, g, sign, send_sem, recv_sem):
        base = g * per_group if g else 0
        for i, (dz, dy) in enumerate(groups[g]):
            for dc in range(nc):
                rows = pl.ds((base + i * nc + dc) * most, most)
                rows = rows if g else (slice(None), rows)
                if dz == dy == dc == 0:
                    assert i == 0
                    continue
                target, arrival, z_off = dst.at[rows], recv_sem.at[g], sign * dz
                if g in far and i < far_offsets:
                    way = 0 if sign == 1 else 1
                    target = relayed.at[way, pl.ds((i * nc + dc) * most, most)]
                    arrival, z_off = relay_recv.at[way], -(nz // 4)
                pltpu.make_async_remote_copy(
                    src_ref=src.at[rows],
                    dst_ref=target,
                    send_sem=send_sem.at[g],
                    recv_sem=arrival,
                    device_id=relative(1, z_off, sign * dy, sign * dc),
                    device_id_type=MESH,
                ).start()
        if g == 0:
            dst[:, 0:most] = src[:, 0:most]

    def exchanged(ref, g, sem):
        rows = pl.ds(g * per_group * most, per_group * most)
        if g == 0:
            rows = (slice(None), pl.ds(most, (per_group - 1) * most))
        with jax.named_scope("wait"):
            pltpu.make_async_copy(ref.at[rows], ref.at[rows], sem.at[g]).wait()

    slots = lax.broadcasted_iota(I32, (gr, t_rows), 0)

    def gather(g):
        s0, s1 = (slots + g * gr == pos0), (slots + g * gr == pos1)
        chosen = (s0.astype(F32) + s1.astype(F32)).astype(BF16)
        rows = jnp.dot(chosen, tokens[...], preferred_element_type=F32)
        rows2d[...] = rows.astype(BF16)
        if g:
            to_tiles(rows2d, out3, g * gr)
        else:
            to_tiles(rows2d, fx.at[0], 0)

    sent = []

    def push(src, dst, send_sem, recv_sem, new_x):
        copy = pltpu.make_async_remote_copy(
            src_ref=src, dst_ref=dst, send_sem=send_sem, recv_sem=recv_sem,
            device_id=at_x(new_x), device_id_type=MESH,
        )
        copy.start()
        sent.append(copy)

    def arrive(ref, sem):
        with jax.named_scope("wait"):
            pltpu.make_async_copy(ref, ref, sem).wait()

    def rows_of(slot):
        return pl.ds(slot * gr, gr)

    def onward(way):
        (g,) = far
        rows = pl.ds(g * per_group * most, far_offsets * nc * most)
        dst, recv_sem = ((recv3, a2a_recv), (back3, back_recv))[way]
        arrive(relayed.at[way], relay_recv.at[way])
        copy = pltpu.make_async_remote_copy(
            src_ref=relayed.at[way], dst_ref=dst.at[rows], send_sem=relay_send.at[way], recv_sem=recv_sem.at[g],
            device_id=relative(1, -(nz // 4), 0, 0), device_id_type=MESH,
        )
        copy.start()
        sent.append(copy)

    def s1(g):
        exchanged(recv3, g, a2a_recv)
        from_tiles(block_in(recv3, g * gr), a2d.at[g])
        me = rows_of(0)
        push(a2d.at[g, me, lo], a2d.at[g, rows_of(1), lo], ag_send.at[g, 0], ag_recv.at[g, 0], right)
        push(a2d.at[g, me, hi], a2d.at[g, rows_of(2), hi], ag_send.at[g, 1], ag_recv.at[g, 1], left)
        push(a2d.at[g, me, hi], a2d.at[g, rows_of(1), hi], ag_send.at[g, 2], ag_recv.at[g, 2], right)
        push(a2d.at[g, me, lo], a2d.at[g, rows_of(2), lo], ag_send.at[g, 3], ag_recv.at[g, 3], left)

    def s2(g):
        arrive(a2d.at[g, rows_of(1), lo], ag_recv.at[g, 0])
        push(a2d.at[g, rows_of(1), lo], a2d.at[g, rows_of(3), lo], ag_send.at[g, 4], ag_recv.at[g, 4], right)
        arrive(a2d.at[g, rows_of(2), hi], ag_recv.at[g, 1])
        push(a2d.at[g, rows_of(2), hi], a2d.at[g, rows_of(3), hi], ag_send.at[g, 5], ag_recv.at[g, 5], left)

    def expert_hidden(g):
        while loads:
            loads.pop().wait()
        rows = a2d[g]
        by_unit = (((1,), (1,)), ((), ()))
        gate = lax.dot_general(rows, wg[...], by_unit, preferred_element_type=F32)
        up = lax.dot_general(rows, wu[...], by_unit, preferred_element_type=F32)
        hid[...] = (gate / (1.0 + jnp.exp(-gate)) * up).astype(BF16)

    def s3(g):
        arrive(a2d.at[g, rows_of(1), hi], ag_recv.at[g, 2])
        arrive(a2d.at[g, rows_of(2), lo], ag_recv.at[g, 3])
        arrive(a2d.at[g, rows_of(3), lo], ag_recv.at[g, 4])
        arrive(a2d.at[g, rows_of(3), hi], ag_recv.at[g, 5])
        expert_hidden(g)
        n_cols = half // 2
        for n in range(4):
            cols = slice(n * n_cols, (n + 1) * n_cols)
            res = jnp.dot(hid[...], wd[:, cols], preferred_element_type=F32)
            own[g, :, cols] = res[0:gr]
            to_left, to_right = res[gr : 2 * gr], res[2 * gr : 3 * gr]
            in_half = slice((n % 2) * n_cols, (n % 2 + 1) * n_cols)
            if n < 2:
                part[g, 0, :, cols] = to_left.astype(BF16)
                pf[g, 1, :, in_half] = to_right
            else:
                pf[g, 0, :, in_half] = to_left
                part[g, 1, :, cols] = to_right.astype(BF16)
            part[g, 2, :, cols] = res[3 * gr : 4 * gr].astype(BF16)
        push(part.at[g, 2, :, lo], rs1.at[g, 0], rs_send.at[g, 0], rs_recv.at[g, 0], right)
        push(part.at[g, 2, :, hi], rs1.at[g, 1], rs_send.at[g, 1], rs_recv.at[g, 1], left)
        push(part.at[g, 1, :, hi], rs2.at[g, 0, :, hi], rs_send.at[g, 2], rs_recv.at[g, 2], right)
        push(part.at[g, 0, :, lo], rs2.at[g, 1, :, lo], rs_send.at[g, 3], rs_recv.at[g, 3], left)

    def s4(g):
        arrive(rs1.at[g, 0], rs_recv.at[g, 0])
        part[g, 1, :, 0:half] = (pf[g, 1] + rs1[g, 0].astype(F32)).astype(BF16)
        push(part.at[g, 1, :, lo], rs2.at[g, 0, :, lo], rs_send.at[g, 4], rs_recv.at[g, 4], right)
        arrive(rs1.at[g, 1], rs_recv.at[g, 1])
        part[g, 0, :, half:width] = (pf[g, 0] + rs1[g, 1].astype(F32)).astype(BF16)
        push(part.at[g, 0, :, hi], rs2.at[g, 1, :, hi], rs_send.at[g, 5], rs_recv.at[g, 5], left)

    def s5(g):
        arrive(rs2.at[g, 0, :, hi], rs_recv.at[g, 2])
        arrive(rs2.at[g, 1, :, lo], rs_recv.at[g, 3])
        arrive(rs2.at[g, 0, :, lo], rs_recv.at[g, 4])
        arrive(rs2.at[g, 1, :, hi], rs_recv.at[g, 5])
        total = own[g] + rs2[g, 0].astype(F32) + rs2[g, 1].astype(F32)
        rows2d[...] = total.astype(BF16)
        to_tiles(rows2d, ret3, g * gr)
        exchange(ret3, back3, g, -1, back_send, back_recv)

    def s6(g):
        exchanged(back3, g, back_recv)
        from_tiles(block_in(back3, g * gr), rows2d)
        combine(g)

    combined = []

    def combine(g):
        rows = rows2d[...]
        res = jnp.dot(whi[g], rows, preferred_element_type=F32)
        res = res + jnp.dot(wlo[g], rows, preferred_element_type=F32)
        combined.append(g)
        if len(combined) == len(groups):
            out[...] = (acc[...] + res).astype(BF16)
        elif len(combined) == 1:
            acc[...] = res
        else:
            acc[...] = acc[...] + res

    top, low = pl.ds(0, gr // 2), pl.ds(gr // 2, gr - gr // 2)

    def n1():
        push(fx.at[0, top], fx.at[1, top], fx_send.at[0], fx_recv.at[0], right)
        push(fx.at[0, low], fx.at[2, low], fx_send.at[1], fx_recv.at[1], left)
        push(fx.at[0, low], fx.at[1, low], fx_send.at[2], fx_recv.at[2], right)
        push(fx.at[0, top], fx.at[2, top], fx_send.at[3], fx_recv.at[3], left)

    def n2():
        arrive(fx.at[1, top], fx_recv.at[0])
        push(fx.at[1, top], fx.at[3, top], fx_send.at[4], fx_recv.at[4], right)
        arrive(fx.at[2, low], fx_recv.at[1])
        push(fx.at[2, low], fx.at[3, low], fx_send.at[5], fx_recv.at[5], left)

    def n3():
        arrive(fx.at[1, low], fx_recv.at[2])
        arrive(fx.at[2, top], fx_recv.at[3])
        arrive(fx.at[3, top], fx_recv.at[4])
        arrive(fx.at[3, low], fx_recv.at[5])
        exchange(fx, fr, 0, 1, a2a_send, a2a_recv)

    def n4():
        exchanged(fr, 0, a2a_recv)
        for k in range(nx):
            from_tiles(block_in(fr.at[k], 0), a2d.at[0, rows_of(k)])
        expert_hidden(0)
        n_cols = width // 4
        for n in range(4):
            cols = slice(n * n_cols, (n + 1) * n_cols)
            a2d[0, :, cols] = jnp.dot(hid[...], wd[:, cols], preferred_element_type=F32).astype(BF16)
        for k in range(nx):
            to_tiles(a2d.at[0, rows_of(k)], fs.at[k], 0)
        exchange(fs, fb, 0, -1, back_send, back_recv)

    def n5():
        exchanged(fb, 0, back_recv)
        push(fb.at[3, top], f1.at[0], fb_send.at[0], fb_recv.at[0], right)
        push(fb.at[3, low], f1.at[1], fb_send.at[1], fb_recv.at[1], left)
        push(fb.at[2, low], f2.at[0, low], fb_send.at[2], fb_recv.at[2], right)
        push(fb.at[1, top], f2.at[1, top], fb_send.at[3], fb_recv.at[3], left)

    def n6():
        arrive(f1.at[0], fb_recv.at[0])
        fsum[0] = (fb[2, top].astype(F32) + f1[0].astype(F32)).astype(BF16)
        push(fsum.at[0], f2.at[0, top], fb_send.at[4], fb_recv.at[4], right)
        arrive(f1.at[1], fb_recv.at[1])
        fsum[1] = (fb[1, low].astype(F32) + f1[1].astype(F32)).astype(BF16)
        push(fsum.at[1], f2.at[1, low], fb_send.at[5], fb_recv.at[5], left)

    def n7():
        arrive(f2.at[0, low], fb_recv.at[2])
        arrive(f2.at[1, top], fb_recv.at[3])
        arrive(f2.at[0, top], fb_recv.at[4])
        arrive(f2.at[1, low], fb_recv.at[5])

        def summed(r):
            rows = slice(r, r + ROW_TILE)
            both = f2[0, rows].astype(F32) + f2[1, rows].astype(F32)
            return (fb[0, rows].astype(F32) + both).astype(BF16)

        from_tiles(summed, rows2d)
        combine(0)

    def send_counts():
        def one(i, carry):
            pltpu.make_async_remote_copy(
                src_ref=cnt_mine, dst_ref=cnt_all.at[i], send_sem=cnt_send, recv_sem=cnt_recv,
                device_id=relative(1, *split(i)), device_id_type=MESH,
            ).start()
            return carry

        lax.fori_loop(1, plane, one, 0)

    counted = {}

    def plane_counts():
        arrive(cnt_all.at[pl.ds(1, plane - 1)], cnt_recv)
        table = cnt_all[:, 0, 0:n_experts]
        i = lax.broadcasted_iota(I32, (plane, 1), 0)
        sz = (z - lax.shift_right_logical(i, log2(per_z)) + nz) & (nz - 1)
        sy = (y - (lax.shift_right_logical(i, log2(nc)) & (ny - 1)) + ny) & (ny - 1)
        sc = (c - (i & (nc - 1)) + nc) & (nc - 1)
        mine = (z * ny + y) * nc + c
        first = ((sz * ny + sy) * nc + sc < mine).astype(F32)
        counted["inside"] = jnp.sum(table * first, axis=0, keepdims=True)
        tot_mine[:, 0:n_experts] = jnp.sum(table, axis=0, keepdims=True)
        for k, new_x in enumerate((right, left, opp)):
            push(tot_mine, tot_all.at[k], tot_send.at[k], tot_recv.at[k], new_x)

    def weigh():
        small[2].wait()
        small[3].wait()
        offset = counted["inside"]
        for k, src in enumerate((left, right, opp)):
            arrive(tot_all.at[k], tot_recv.at[k])
            offset = offset + tot_all[k][:, 0:n_experts] * jnp.where(src < x, 1.0, 0.0)
        diagonal = lax.broadcasted_iota(I32, (n_experts, n_experts), 0) == lax.broadcasted_iota(
            I32, (n_experts, n_experts), 1
        )

        def down(row):
            return jnp.sum(jnp.where(diagonal, row, 0.0), axis=1, keepdims=True)

        offset, limit = down(offset), down(cap[...].astype(F32))
        parts = []
        for k, (oh, rank, pos) in enumerate(((oh0, rank0, pos0), (oh1, rank1, pos1))):
            slot = jnp.sum(oh * offset, axis=0, keepdims=True) + rank
            top = jnp.sum(oh * limit, axis=0, keepdims=True)
            unit = jnp.where(slot < top, units[k : k + 1, :], 0)
            high = unit & ~7
            parts.append((pos, high.astype(F32) / 1024.0, (unit - high).astype(F32) / 1024.0))
        wide = lax.broadcasted_iota(I32, (LANES, t_rows), 0)
        for g in range(len(groups)):
            h = l = jnp.zeros((LANES, t_rows), F32)
            for pos, high, low in parts:
                here = wide + g * gr == pos
                h, l = h + jnp.where(here, high, 0.0), l + jnp.where(here, low, 0.0)
            whi[g] = jnp.transpose(h)[:, 0:gr].astype(BF16)
            wlo[g] = jnp.transpose(l)[:, 0:gr].astype(BF16)

    n = len(groups)
    steps = nz // 2 - 1

    def dispatch(g):
        gather(g)
        exchange(out3, recv3, g, 1, a2a_send, a2a_recv)

    def enter():
        gather(0)
        with jax.named_scope("barrier"):
            near_ready()

    def relay(step):
        told(step)
        if step + 1 < steps:
            tell(step + 1)

    if n == 4:
        order = [
            (enter,), (n1,), (tell, 0), (relay, 0), (dispatch, 3), (relay, 1), (n2,), (relay, 2), (dispatch, 1),
            (s1, 3), (dispatch, 2), (s2, 3), (s1, 1), (send_counts,), (onward, 0), (s2, 1), (n3,), (s1, 2), (s3, 1),
            (s2, 2), (s4, 1), (n4,), (s3, 2), (s5, 1), (plane_counts,), (s4, 2), (s3, 3), (s5, 2), (s4, 3), (n5,),
            (weigh,), (onward, 1), (s5, 3), (s6, 1), (n6,), (s6, 2), (n7,), (s6, 3),
        ]
    else:
        order = [(enter,), (n1,), (tell, 0)] + [(relay, step) for step in range(steps)]
        order += [(dispatch, g) for g in range(1, n)] + [(n2,), (n3,), (onward, 0)]
        order += [(stage, g) for stage in (s1, s2, s3, s4, s5) for g in range(1, n)]
        order += [(n4,), (send_counts,), (plane_counts,), (weigh,), (n5,), (n6,), (onward, 1)] + [(s6, g) for g in range(1, n)] + [(n7,)]
    for stage, *args in order:
        with jax.named_scope("_".join([stage.__name__, *map(str, args)])):
            stage(*args)

    for copy in sent:
        copy.wait_send()
    exchanged(fx, 0, a2a_send)
    exchanged(fs, 0, back_send)
    for g in range(1, n):
        exchanged(out3, g, a2a_send)
        exchanged(ret3, g, back_send)
    arrive(cnt_all.at[pl.ds(1, plane - 1)], cnt_send)


def local(shape, most, tokens, expert_ids, gate_units, capacity, w_gate, w_up, w_down):
    nx, nz, ny, nc = shape
    t_rows, width = tokens.shape
    ff = w_gate.shape[2]
    turn = functools.partial(jnp.swapaxes, axis1=-1, axis2=-2)
    plane = nz * ny * nc
    groups = offset_groups(nz, ny)
    n, gr = len(groups), len(groups[0]) * nc * most
    vmem = pl.BlockSpec(memory_space=pltpu.VMEM)
    in_hbm = pl.BlockSpec(memory_space=pltpu.HBM)
    stay = functools.partial(pltpu.with_memory_space_constraint, memory_space=pltpu.HBM)
    dma = pltpu.SemaphoreType.DMA
    near_tiles = pltpu.VMEM((nx, gr, ROW_TILE, LANES), BF16)
    tiles = pltpu.VMEM((plane * most, ROW_TILE, LANES), BF16)
    return pl.pallas_call(
        functools.partial(kernel, shape, most),
        out_shape=jax.ShapeDtypeStruct((t_rows, width), BF16),
        in_specs=[in_hbm] * 7,
        out_specs=vmem,
        scratch_shapes=[
            pltpu.VMEM((t_rows, width), BF16),
            pltpu.VMEM((2, t_rows), I32),
            pltpu.VMEM((2, t_rows), I32),
            pltpu.VMEM((1, plane), I32),
            pltpu.VMEM((ff, width), BF16),
            pltpu.VMEM((ff, width), BF16),
            pltpu.VMEM((ff, width), BF16),
            pltpu.VMEM((256, 256), BF16),
            pltpu.VMEM((gr, width), BF16),
            tiles, tiles, tiles, tiles,
            pltpu.VMEM((n, nx * gr, width), BF16),
            pltpu.VMEM((nx * gr, ff), BF16),
            pltpu.VMEM((n, gr, width), F32),
            pltpu.VMEM((n, 2, gr, width // 2), F32),
            pltpu.VMEM((n, 3, gr, width), BF16),
            pltpu.VMEM((n, 2, gr, width // 2), BF16),
            pltpu.VMEM((n, 2, gr, width), BF16),
            pltpu.VMEM((8, LANES), F32),
            pltpu.VMEM((n, t_rows, gr), BF16),
            pltpu.VMEM((n, t_rows, gr), BF16),
            pltpu.VMEM((t_rows, width), F32),
            pltpu.VMEM((1, LANES), F32),
            pltpu.VMEM((plane, 1, LANES), F32),
            pltpu.VMEM((1, LANES), F32),
            pltpu.VMEM((3, 1, LANES), F32),
            near_tiles, near_tiles, near_tiles, near_tiles,
            pltpu.VMEM((2, gr // 2, ROW_TILE, LANES), BF16),
            pltpu.VMEM((2, gr, ROW_TILE, LANES), BF16),
            pltpu.VMEM((2, gr // 2, ROW_TILE, LANES), BF16),
            pltpu.VMEM((2, min(2, ny) * nc * most, ROW_TILE, LANES), BF16),
            pltpu.SemaphoreType.REGULAR((nz // 2 - 1,)),
            dma((7,)),
            dma((n,)), dma((n,)),
            dma((n, 6)), dma((n, 6)),
            dma((n, 6)), dma((n, 6)),
            dma((n,)), dma((n,)),
            dma, dma,
            dma((3,)), dma((3,)),
            dma((6,)), dma((6,)),
            dma((6,)), dma((6,)),
            dma((2,)), dma((2,)),
        ],
        compiler_params=pltpu.CompilerParams(collective_id=0, has_side_effects=True, vmem_limit_bytes=56000000),
    )(
        tokens, stay(turn(expert_ids)), stay(turn(gate_units)), stay(capacity.reshape(1, -1)),
        turn(w_gate), turn(w_up), turn(w_down),
    )


def build(finer, most):
    shape = tuple(finer.shape[a] for a in AXES)
    return jax.shard_map(
        functools.partial(local, shape, most),
        mesh=finer,
        in_specs=(
            P(AXES, None),
            P(AXES, None),
            P(AXES, None),
            P(),
            P(EXPERT, None, "dp"),
            P(EXPERT, None, "dp"),
            P(EXPERT, None, "dp"),
        ),
        out_specs=P(AXES, None),
        check_vma=False,
    )


def solution(mesh):
    finer = Mesh(mesh.devices.reshape(mesh.shape["dp"], 8, 4, 2), AXES)
    return build(finer, 5)
```
